256 devices in a mesh: row: 64 (over y, x, z_hi), ka: 4 (over z_lo, core).
Axes of the slice: x: 4, y: 4, z: 8 (z_hi: 4, z_lo: 2; z = z_hi * 2 + z_lo), core: 2. Of those that a mesh axis runs over, the one named last changes fastest.
Arguments:
- pair_rep: bfloat16 [256, 256, 128], P('row', 'ka'), may hold values from -6 to 6
- in_weights: bfloat16 [2, 128, 512], replicated, may hold values from -0.5 to 0.5
- gate_weights: bfloat16 [2, 128, 128], replicated, may hold values from -0.5 to 0.5
- out_weights: bfloat16 [2, 128, 128], replicated, may hold values from -0.5 to 0.5
Outputs:
- refined: bfloat16 [256, 256, 128], P('row', 'ka')
The draws below stay inside these ranges and needn't reach their ends.
All inputs are finite; a program needn't handle non-finite values.
Results may differ from the reference program's by a relative error of at most 0.015.
Values may be sent and summed in bfloat16 or wider, within the bound.
No kernel may reach another device: no remote copies, remote signals or barrier semaphores. Data moves between devices by JAX's collectives and lax.ppermute only.
A program may use at most 64 MiB of HBM per device.

```python
import jax
import jax.numpy as jnp
from jax import lax

PAIR_CH = 128
TRI_CH = 128
N = 256


def level_of(key, dims, pieces, least, high):
    def one(axis_at, parts):
        steps = jax.random.uniform(jax.random.fold_in(jax.random.fold_in(key, 6), axis_at), (parts,), jnp.float32, least / len(pieces), high / len(pieces))
        return jnp.repeat(jnp.exp(steps), dims[axis_at] // parts).reshape((-1,) + (1,) * (len(dims) - axis_at - 1))

    factor_of = one(*pieces[0])
    for cut in pieces[1:]:
        factor_of = factor_of * one(*cut)
    return factor_of


def scatter_about(rng, extent, scale, limit, split=(), dtype=jnp.bfloat16):
    factor_of = level_of(rng, extent, split, -0.22, 0.18) if split else 1.0
    array = jax.random.normal(rng, extent, jnp.float32) * scale * factor_of
    return jnp.minimum(jnp.maximum(array, -limit), limit).astype(dtype)


def setup_inputs(seed: int = 0) -> dict:
    keys = jax.random.split(jax.random.key(seed), 5)
    pair_rep = scatter_about(keys[0], (N, N, PAIR_CH), 1.0, 6.0, ((0, 64), (1, 4)))
    in_weights = scatter_about(keys[1], (2, PAIR_CH, 4 * TRI_CH), PAIR_CH ** -0.5, 0.5)
    gate_weights = scatter_about(keys[2], (2, PAIR_CH, PAIR_CH), PAIR_CH ** -0.5, 0.5)
    out_weights = scatter_about(keys[3], (2, TRI_CH, PAIR_CH), TRI_CH ** -0.5, 0.5)
    return {"pair_rep": pair_rep, "in_weights": in_weights, "gate_weights": gate_weights, "out_weights": out_weights}


EPSILON = 1e-05

def layer_norm(values):
    values = values.astype(jnp.float32)
    centre = lax.optimization_barrier(jnp.mean(values, axis=-1, keepdims=True))
    shifted = values - centre
    spread = lax.optimization_barrier(jnp.mean(shifted * shifted, axis=-1, keepdims=True))
    return shifted * jax.lax.rsqrt(spread + EPSILON)

def reference(pair_rep, in_weights, gate_weights, out_weights):
    state = pair_rep
    for section in range(2):
        normed = layer_norm(state).astype(jnp.bfloat16)
        flattened = normed.reshape(-1, PAIR_CH)
        projected = jnp.dot(flattened, in_weights[section], preferred_element_type=jnp.float32)
        left_rows = (jax.nn.sigmoid(projected[:, :TRI_CH]) * projected[:, TRI_CH:2 * TRI_CH]).astype(jnp.bfloat16)
        right_rows = (jax.nn.sigmoid(projected[:, 2 * TRI_CH:3 * TRI_CH]) * projected[:, 3 * TRI_CH:]).astype(jnp.bfloat16)
        left_rows = left_rows.reshape(N, N, TRI_CH)
        right_rows = right_rows.reshape(N, N, TRI_CH)
        gating = jax.nn.sigmoid(jnp.dot(flattened, gate_weights[section], preferred_element_type=jnp.float32))
        gating = gating.reshape(N, N, PAIR_CH)
        if section == 1:
            left_rows = jnp.transpose(left_rows, (1, 0, 2))
            right_rows = jnp.transpose(right_rows, (1, 0, 2))
        product = jnp.einsum('ikh,jkh->ijh', left_rows.astype(jnp.float32), right_rows.astype(jnp.float32))
        squeezed = layer_norm(product).astype(jnp.bfloat16).reshape(-1, TRI_CH)
        update = jnp.dot(squeezed, out_weights[section], preferred_element_type=jnp.float32).reshape(N, N, PAIR_CH)
        state = (state.astype(jnp.float32) + gating * update).astype(jnp.bfloat16)
    return state
```

```python
import jax
import jax.numpy as jnp
from jax import lax
from jax.experimental import pallas as pl
from jax.experimental.pallas import tpu as pltpu
from jax.sharding import Mesh, PartitionSpec as P

EPSILON = 1e-05
BF16 = jnp.bfloat16
F32 = jnp.float32

CHIPS = ("zl", "y", "x", "zh")


def nn(a, b):
    return lax.dot_general(a, b, (((1,), (0,)), ((), ())), preferred_element_type=F32)


def nt(a, b):
    return lax.dot_general(a, b, (((1,), (1,)), ((), ())), preferred_element_type=F32)


def picks(rows, cols, source):
    row = lax.broadcasted_iota(jnp.int32, (rows, cols), 0)
    col = lax.broadcasted_iota(jnp.int32, (rows, cols), 1)
    return (col == source(row)).astype(F32).astype(BF16)


def moved(one_hot, values):
    return nn(one_hot, values).astype(BF16)


def interleaved(parts, per_block):
    count = len(parts)
    size = count * per_block
    shuffle = picks(size, size, lambda i: i % count * per_block + i // count)
    blocks = []
    for start in range(0, parts[0].shape[0], per_block):
        stacked = jnp.concatenate([p[start : start + per_block] for p in parts], 0)
        blocks.append(moved(shuffle, stacked))
    return jnp.concatenate(blocks, 0)


def normalized(values):
    shifted = values - jnp.mean(values, axis=0, keepdims=True)
    spread = jnp.mean(shifted * shifted, axis=0, keepdims=True)
    return (shifted * lax.rsqrt(spread + EPSILON)).astype(BF16)


def sigmoid(x):
    return 1.0 / (1.0 + jnp.exp(-x))


def operands(weights, normed):
    projected = nn(weights, normed)
    left = sigmoid(projected[0:128]) * projected[128:256]
    right = sigmoid(projected[256:384]) * projected[384:512]
    return left.astype(BF16), right.astype(BF16)


def halves_swapped(a, b):
    low = lax.broadcasted_iota(jnp.int32, a.shape, 1) < 64
    rolled_a, rolled_b = jnp.roll(a, 64, 1), jnp.roll(b, 64, 1)
    return jnp.where(low, a, rolled_b), jnp.where(low, rolled_a, b)


def identity(size):
    return picks(size, size, lambda i: i)


def first_math(core, own, partner, in_w, gate_w):
    own_t = nt(identity(128), own)
    partner_t = nt(identity(128), partner)
    gate = sigmoid(nn(gate_w, normalized(own_t)))
    pieces = []
    for pair in range(2):
        mine = own_t[:, 128 * pair : 128 * pair + 128]
        other = partner_t[:, 128 * pair : 128 * pair + 128]
        lo = jnp.where(core == 0, mine, other)
        hi = jnp.where(core == 0, other, mine)
        pieces.extend(halves_swapped(lo, hi))
    both = jnp.concatenate(pieces, 1)
    left, right = operands(in_w, normalized(both))
    parts = [v[:, 128 * r : 128 * r + 128] for v in (left, right) for r in range(4)]
    return interleaved(parts, 32), own_t, gate


def returned(total_even, total_odd):
    out = halves_swapped(total_even, total_odd)
    return jnp.concatenate(out, 0).astype(BF16)


def outgoing_math(core, received):
    take_left = picks(256, 512, lambda i: i % 128 // 2 * 8 + i % 2 * 2 + i // 128)
    take_right = picks(
        128, 512, lambda j: (j // 64 * 32 + core * 16 + j % 64 // 4) * 8 + 4 + j % 4
    )
    total = 0.0
    for zl in range(2):
        block = received[512 * zl : 512 * zl + 512]
        total += nt(moved(take_left, block), moved(take_right, block))
    return returned(total[0:128], total[128:256])


def residual(gathered, out_w, state, gate):
    split = nn(picks(256, 256, lambda i: i % 128 * 2 + i // 128), gathered)
    product = jnp.concatenate([split[0:128], split[128:256]], 1)
    return (state + gate * nn(out_w, normalized(product))).astype(BF16)


def middle_math(gathered, state, gate, out_w, in_w, gate_w):
    middle = residual(gathered, out_w, state, gate).astype(F32)
    normed = normalized(middle)
    left, right = operands(in_w, normed)
    next_gate = sigmoid(nn(gate_w, normed))
    parts = [v[:, 128 * r : 128 * r + 128] for v in (left, right) for r in range(2)]
    return interleaved(parts, 64), middle, next_gate


def incoming_math(core, received, partner_left):
    take_left = picks(128, 256, lambda i: i // 2 * 4 + i % 2)
    take_right = picks(128, 256, lambda i: i // 2 * 4 + 2 + i % 2)
    lanes = picks(128, 128, lambda i: i // 64 * 64 + i % 32 * 2 + i % 64 // 32)
    lefts, rights = {}, []
    for zl in range(2):
        block = received[256 * zl : 256 * zl + 256]
        mine = nt(lanes, moved(take_left, block)).astype(BF16)
        other = nt(lanes, partner_left[128 * zl : 128 * zl + 128]).astype(BF16)
        lefts[zl, 0] = jnp.where(core == 0, mine, other)
        lefts[zl, 1] = jnp.where(core == 0, other, mine)
        rights.append(nn(take_right, block))
    right = jnp.concatenate(halves_swapped(*rights), 0).astype(BF16)
    order = [lefts[zl, c] for zl in range(2) for c in range(2)]
    totals = []
    for odd in range(2):
        rows = [
            jnp.concatenate([v[32 * odd : 32 * odd + 32], v[64 + 32 * odd : 96 + 32 * odd]], 1)
            for v in order
        ]
        totals.append(nn(jnp.concatenate(rows, 0), right))
    return returned(*totals)


def last_math(gathered, state, gate, out_w):
    refined = residual(gathered, out_w, state, gate)
    return nt(identity(256), refined).astype(BF16)


def first_kernel(core, own, partner, in_w, gate_w, sent, state, gate):
    sent[...], state[...], gate[...] = first_math(
        core[0], own[...], partner[...], in_w[...], gate_w[...]
    )


def outgoing_kernel(core, received, sent):
    sent[...] = outgoing_math(core[0], received[...])


def middle_kernel(gathered, state, gate, out_w, in_w, gate_w, sent, middle, next_gate):
    sent[...], middle[...], next_gate[...] = middle_math(
        gathered[...], state[...], gate[...], out_w[...], in_w[...], gate_w[...]
    )


def incoming_kernel(core, received, partner_left, sent):
    sent[...] = incoming_math(core[0], received[...], partner_left[...])


def last_kernel(gathered, state, gate, out_w, refined):
    refined[...] = last_math(gathered[...], state[...], gate[...], out_w[...])


def call(kernel, outs, scalars, *arrays):
    smem = pl.BlockSpec(memory_space=pltpu.SMEM)
    vmem = pl.BlockSpec(memory_space=pltpu.VMEM)
    shapes = tuple(jax.ShapeDtypeStruct(shape, dtype) for shape, dtype in outs)
    return pl.pallas_call(
        kernel,
        out_shape=shapes,
        in_specs=[smem] * len(scalars) + [vmem] * len(arrays),
        out_specs=tuple(vmem for _ in shapes),
    )(*scalars, *arrays)


def exchanged(rows, per_chip):
    blocks = rows.reshape(128, per_chip, 128)
    return lax.all_to_all(blocks, CHIPS, 0, 0, tiled=True)


def from_partner(value):
    return lax.ppermute(value, "c", [(0, 1), (1, 0)])


def per_device(pair_rep, in_weights, gate_weights, out_weights):
    core = lax.axis_index("c").astype(jnp.int32).reshape(1)
    own = pair_rep.reshape(256, 128)
    partner = from_partner(own)
    in_w = jnp.swapaxes(in_weights, 1, 2)
    gate_w = jnp.swapaxes(gate_weights, 1, 2)
    out_w = jnp.swapaxes(out_weights, 1, 2)
    state_like = ((128, 256), F32)
    sent, state, gate = call(
        first_kernel, [((1024, 128), BF16), state_like, state_like], (core,),
        own, partner, in_w[0], gate_w[0],
    )
    received = exchanged(sent, 8).reshape(1024, 128)
    (sent,) = call(outgoing_kernel, [((256, 128), BF16)], (core,), received)
    gathered = exchanged(sent, 2).reshape(256, 128)
    sent, middle, gate = call(
        middle_kernel, [((512, 128), BF16), state_like, state_like], (),
        gathered, state, gate, out_w[0], in_w[1], gate_w[1],
    )
    received = exchanged(sent, 4)
    partner_left = from_partner(received[:, 0:2]).reshape(256, 128)
    (sent,) = call(
        incoming_kernel, [((256, 128), BF16)], (core,), received.reshape(512, 128), partner_left
    )
    gathered = exchanged(sent, 2).reshape(256, 128)
    (refined,) = call(last_kernel, [((256, 128), BF16)], (), gathered, middle, gate, out_w[1])
    return refined.reshape(pair_rep.shape)


def solution(mesh):
    fine = Mesh(mesh.devices.reshape(4, 4, 4, 2, 2), ("y", "x", "zh", "zl", "c"))
    placed = P(("y", "x", "zh"), ("zl", "c"), None)
    return jax.shard_map(
        per_device, mesh=fine, in_specs=(placed, P(), P(), P()), out_specs=placed, check_vma=False
    )
```

```python
import jax
import jax.numpy as jnp
from jax import lax
from jax.experimental import pallas as pl
from jax.experimental.pallas import tpu as pltpu
from jax.sharding import Mesh, PartitionSpec as P

EPSILON = 1e-05
BF16 = jnp.bfloat16
F32 = jnp.float32

CHIPS = ("zl", "y", "x", "zh")


def nn(a, b):
    return lax.dot_general(a, b, (((1,), (0,)), ((), ())), preferred_element_type=F32)


def nt(a, b):
    return lax.dot_general(a, b, (((1,), (1,)), ((), ())), preferred_element_type=F32)


def picks(rows, cols, source):
    row = lax.broadcasted_iota(jnp.int32, (rows, cols), 0)
    col = lax.broadcasted_iota(jnp.int32, (rows, cols), 1)
    return (col == source(row)).astype(F32).astype(BF16)


def moved(one_hot, values):
    return nn(one_hot, values).astype(BF16)


def interleaved(parts, per_block):
    count = len(parts)
    size = count * per_block
    shuffle = picks(size, size, lambda i: i % count * per_block + i // count)
    blocks = []
    for start in range(0, parts[0].shape[0], per_block):
        stacked = jnp.concatenate([p[start : start + per_block] for p in parts], 0)
        blocks.append(moved(shuffle, stacked))
    return jnp.concatenate(blocks, 0)


def normalized(values):
    shifted = values - jnp.mean(values, axis=0, keepdims=True)
    spread = jnp.mean(shifted * shifted, axis=0, keepdims=True)
    return (shifted * lax.rsqrt(spread + EPSILON)).astype(BF16)


def sigmoid(x):
    return 1.0 / (1.0 + jnp.exp(-x))


def operands(weights, normed):
    projected = nn(weights, normed)
    left = sigmoid(projected[0:128]) * projected[128:256]
    right = sigmoid(projected[256:384]) * projected[384:512]
    return left.astype(BF16), right.astype(BF16)


def halves_swapped(a, b):
    low = lax.broadcasted_iota(jnp.int32, a.shape, 1) < 64
    rolled_a, rolled_b = jnp.roll(a, 64, 1), jnp.roll(b, 64, 1)
    return jnp.where(low, a, rolled_b), jnp.where(low, rolled_a, b)


def identity(size):
    return picks(size, size, lambda i: i)


def transposed(weights):
    eye = identity(128)
    blocks = [nt(eye, weights[:, k : k + 128]) for k in range(0, weights.shape[1], 128)]
    return jnp.concatenate(blocks, 0).astype(BF16)


def sent_operands(weights, normed):
    left, right = operands(transposed(weights), normed)
    parts = [v[:, 128 * r : 128 * r + 128] for v in (left, right) for r in range(2)]
    return interleaved(parts, 64)


def first_math(own, in_w, gate_w):
    state = nt(identity(128), own)
    normed = normalized(state)
    return sent_operands(in_w, normed), state, sigmoid(nn(transposed(gate_w), normed))


def by_core(core, mine, other):
    return jnp.where(core == 0, mine, other), jnp.where(core == 0, other, mine)


def returned(total_even, total_odd):
    out = halves_swapped(total_even, total_odd)
    return jnp.concatenate(out, 0).astype(BF16)


def outgoing_math(core, received, partner):
    take_left = picks(128, 256, lambda i: i // 2 * 4 + i % 2)
    take_right = picks(64, 256, lambda j: (j // 32 * 32 + core * 16 + j % 32 // 2) * 4 + 2 + j % 2)
    ordered = picks(128, 128, lambda j: j % 2 * 64 + j // 2)
    lefts, rights = ([], []), ([], [])
    for zl in range(2):
        mine = received[256 * zl : 256 * zl + 256]
        other = partner[256 * zl : 256 * zl + 256]
        for take, rows in ((take_left, lefts), (take_right, rights)):
            pair = by_core(core, nn(take, mine), nn(take, other))
            for r, half in enumerate(halves_swapped(*pair)):
                rows[r].append(half.astype(BF16))
    right = jnp.concatenate([jnp.concatenate(v, 1) for v in rights], 0)
    right = moved(ordered, right)
    return returned(*(nt(jnp.concatenate(v, 1), right) for v in lefts))


def residual(gathered, out_w, state, gate):
    split = nn(picks(256, 256, lambda i: i % 128 * 2 + i // 128), gathered)
    product = jnp.concatenate([split[0:128], split[128:256]], 1)
    update = nn(transposed(out_w), normalized(product))
    return (state + gate * update).astype(BF16)


def middle_math(gathered, state, gate, out_w, in_w, gate_w):
    middle = residual(gathered, out_w, state, gate).astype(F32)
    normed = normalized(middle)
    return sent_operands(in_w, normed), middle, sigmoid(nn(transposed(gate_w), normed))


def incoming_math(core, received, partner):
    take_left = picks(128, 256, lambda i: i // 2 * 4 + i % 2)
    take_right = picks(128, 256, lambda i: i // 2 * 4 + 2 + i % 2)
    lanes = picks(128, 128, lambda i: i // 64 * 64 + i % 32 * 2 + i % 64 // 32)
    lefts, rights = {}, []
    for zl in range(2):
        block = received[256 * zl : 256 * zl + 256]
        mine = nt(lanes, moved(take_left, block)).astype(BF16)
        there = moved(take_left, partner[256 * zl : 256 * zl + 256])
        other = nt(lanes, there).astype(BF16)
        lefts[zl, 0], lefts[zl, 1] = by_core(core, mine, other)
        rights.append(nn(take_right, block))
    right = jnp.concatenate(halves_swapped(*rights), 0).astype(BF16)
    order = [lefts[zl, c] for zl in range(2) for c in range(2)]
    totals = []
    for odd in range(2):
        rows = [
            jnp.concatenate([v[32 * odd : 32 * odd + 32], v[64 + 32 * odd : 96 + 32 * odd]], 1)
            for v in order
        ]
        totals.append(nn(jnp.concatenate(rows, 0), right))
    return returned(*totals)


def last_math(gathered, state, gate, out_w):
    refined = residual(gathered, out_w, state, gate)
    return nt(identity(256), refined).astype(BF16)


def first_kernel(own, in_w, gate_w, sent, state, gate):
    sent[...], state[...], gate[...] = first_math(own[...], in_w[0], gate_w[0])


def outgoing_kernel(received, partner, sent):
    sent[...] = outgoing_math(lax.axis_index("c"), received[...], partner[...])


def middle_kernel(gathered, state, gate, out_w, in_w, gate_w, sent, middle, next_gate):
    sent[...], middle[...], next_gate[...] = middle_math(
        gathered[...], state[...], gate[...], out_w[0], in_w[1], gate_w[1]
    )


def incoming_kernel(received, partner, sent):
    sent[...] = incoming_math(lax.axis_index("c"), received[...], partner[...])


def last_kernel(gathered, state, gate, out_w, refined):
    refined[...] = last_math(gathered[...], state[...], gate[...], out_w[1])


def call(kernel, outs, *arrays):
    vmem = pl.BlockSpec(memory_space=pltpu.VMEM)
    return pl.pallas_call(
        kernel,
        out_shape=tuple(jax.ShapeDtypeStruct(shape, dtype) for shape, dtype in outs),
        in_specs=[vmem] * len(arrays),
        out_specs=tuple(vmem for _ in outs),
        compiler_params=pltpu.CompilerParams(vmem_limit_bytes=16 << 20),
    )(*arrays)


def exchanged(rows):
    blocks = rows.reshape(128, -1, 128)
    return lax.all_to_all(blocks, CHIPS, 0, 0, tiled=True).reshape(rows.shape)


def from_partner(value):
    return lax.ppermute(value, "c", [(0, 1), (1, 0)])


def per_device(pair_rep, in_weights, gate_weights, out_weights):
    own = pair_rep.reshape(256, 128)
    operands_out, results_out = ((512, 128), BF16), ((256, 128), BF16)
    kept = ((128, 256), F32)
    sent, state, gate = call(
        first_kernel, [operands_out, kept, kept], own, in_weights, gate_weights
    )
    received = exchanged(sent)
    (sent,) = call(outgoing_kernel, [results_out], received, from_partner(received))
    sent, state, gate = call(
        middle_kernel, [operands_out, kept, kept],
        exchanged(sent), state, gate, out_weights, in_weights, gate_weights,
    )
    received = exchanged(sent)
    (sent,) = call(incoming_kernel, [results_out], received, from_partner(received))
    (refined,) = call(last_kernel, [results_out], exchanged(sent), state, gate, out_weights)
    return refined.reshape(pair_rep.shape)


def solution(mesh):
    fine = Mesh(mesh.devices.reshape(4, 4, 4, 2, 2), ("y", "x", "zh", "zl", "c"))
    placed = P(("y", "x", "zh"), ("zl", "c"), None)
    return jax.shard_map(
        per_device, mesh=fine, in_specs=(placed, P(), P(), P()), out_specs=placed, check_vma=False
    )
```

```python
import jax
import jax.numpy as jnp
from jax import lax
from jax.experimental import pallas as pl
from jax.experimental.pallas import tpu as pltpu
from jax.sharding import Mesh, PartitionSpec as P

EPSILON = 1e-05
BF16 = jnp.bfloat16
F32 = jnp.float32

CHIPS = ("zl", "y", "x", "zh")
LAYER = ("y", "x", "zl", "c")
ALL = ("zh", "zl", "c", "y", "x")


def nn(a, b):
    return lax.dot_general(a, b, (((1,), (0,)), ((), ())), preferred_element_type=F32)


def nt(a, b):
    return lax.dot_general(a, b, (((1,), (1,)), ((), ())), preferred_element_type=F32)


def picks(rows, cols, source):
    row = lax.broadcasted_iota(jnp.int32, (rows, cols), 0)
    col = lax.broadcasted_iota(jnp.int32, (rows, cols), 1)
    return (col == source(row)).astype(F32).astype(BF16)


def moved(one_hot, values):
    return nn(one_hot, values).astype(BF16)


def interleaved(parts, per_block):
    count = len(parts)
    size = count * per_block
    shuffle = picks(size, size, lambda i: i % count * per_block + i // count)
    blocks = []
    for start in range(0, parts[0].shape[0], per_block):
        stacked = jnp.concatenate([p[start : start + per_block] for p in parts], 0)
        blocks.append(moved(shuffle, stacked))
    return jnp.concatenate(blocks, 0)


def normalized(values):
    shifted = values - jnp.mean(values, axis=0, keepdims=True)
    spread = jnp.mean(shifted * shifted, axis=0, keepdims=True)
    return (shifted * lax.rsqrt(spread + EPSILON)).astype(BF16)


def sigmoid(x):
    return 1.0 / (1.0 + jnp.exp(-x))


def operands(weights, normed):
    projected = nn(weights, normed)
    left = sigmoid(projected[0:128]) * projected[128:256]
    right = sigmoid(projected[256:384]) * projected[384:512]
    return left.astype(BF16), right.astype(BF16)


def halves_swapped(a, b):
    low = lax.broadcasted_iota(jnp.int32, a.shape, 1) < 64
    rolled_a, rolled_b = jnp.roll(a, 64, 1), jnp.roll(b, 64, 1)
    return jnp.where(low, a, rolled_b), jnp.where(low, rolled_a, b)


def identity(size):
    return picks(size, size, lambda i: i)


def transposed(weights):
    eye = identity(128)
    blocks = [nt(eye, weights[:, k : k + 128]) for k in range(0, weights.shape[1], 128)]
    return jnp.concatenate(blocks, 0).astype(BF16)


def sent_operands(weights, normed):
    weights = transposed(weights)
    pairs = [operands(weights, normed[128 * r : 128 * r + 128]) for r in range(2)]
    return interleaved([pair[side] for side in range(2) for pair in pairs], 64)


def gated(weights, normed):
    weights = transposed(weights)
    return jnp.concatenate(
        [sigmoid(nn(weights, normed[128 * r : 128 * r + 128])) for r in range(2)], 0
    )


def normalized_halves(values):
    return jnp.concatenate([normalized(values[0:128]), normalized(values[128:256])], 0)


def normalized_mixed(values):
    def mean(array):
        total = jnp.sum(array, axis=0)
        total = total + jnp.roll(total, 4, 0)
        return (total + jnp.roll(total, 2, 0)) / 128

    tiles = values.reshape(32, 8, 128)
    shifted = tiles - mean(tiles)
    scale = lax.rsqrt(mean(shifted * shifted) + EPSILON)
    return (shifted * scale).reshape(256, 128).astype(BF16)


def first_math(own, in_w, gate_w):
    eye = identity(128)
    state = jnp.concatenate([nt(eye, own[0:128]), nt(eye, own[128:256])], 0)
    normed = normalized_halves(state)
    return sent_operands(in_w, normed), state, gated(gate_w, normed)


def by_core(core, mine, other):
    return jnp.where(core == 0, mine, other), jnp.where(core == 0, other, mine)


def returned(total_even, total_odd):
    out = halves_swapped(total_even, total_odd)
    return jnp.concatenate(out, 0).astype(BF16)


def outgoing_math(core, received, partner):
    take_left = picks(128, 256, lambda i: i // 2 * 4 + i % 2)
    take_right = picks(64, 256, lambda j: (j // 32 * 32 + core * 16 + j % 32 // 2) * 4 + 2 + j % 2)
    ordered = picks(128, 128, lambda j: j % 2 * 64 + j // 2)
    lefts, rights = ([], []), ([], [])
    for zl in range(2):
        mine = received[256 * zl : 256 * zl + 256]
        other = partner[256 * zl : 256 * zl + 256]
        for take, rows in ((take_left, lefts), (take_right, rights)):
            pair = by_core(core, nn(take, mine), nn(take, other))
            for r, half in enumerate(halves_swapped(*pair)):
                rows[r].append(half.astype(BF16))
    right = jnp.concatenate([jnp.concatenate(v, 1) for v in rights], 0)
    right = moved(ordered, right)
    return returned(*(nt(jnp.concatenate(v, 1), right) for v in lefts))


def residual(product, channel_of, out_w, state, gate):
    weights = transposed(out_w)
    row = lax.broadcasted_iota(jnp.int32, (128, 256), 0)
    col = lax.broadcasted_iota(jnp.int32, (128, 256), 1)
    spread = []
    for r in range(2):
        one_hot = (row == channel_of(col // 2)) & (col % 2 == r)
        spread.append(moved(weights, one_hot.astype(F32).astype(BF16)))
    update = nn(jnp.concatenate(spread, 0), normalized_mixed(product))
    return (state + gate * update).astype(BF16)


def middle_math(gathered, state, gate, out_w, in_w, gate_w):
    middle = residual(gathered.astype(F32), lambda h: h, out_w, state, gate).astype(F32)
    normed = normalized_halves(middle)
    return sent_operands(in_w, normed), middle, gated(gate_w, normed)


def incoming_math(received):
    sides = {}
    for channel in range(2):
        for side in range(2):
            place = 4 * channel + 2 * side
            take = picks(128, 512, lambda i: i % 32 // 2 * 32 + i // 32 * 8 + place + i % 2)
            rows = nn(take, received)
            halves = []
            for zl in range(2):
                pair = (rows[64 * zl : 64 * zl + 32], rows[64 * zl + 32 : 64 * zl + 64])
                halves.append(jnp.concatenate(halves_swapped(*pair), 0))
            sides[channel, side] = jnp.concatenate(halves, 1).astype(BF16)
    lefts = []
    for channel in range(2):
        row = lax.broadcasted_iota(jnp.int32, (512, 256), 0)
        col = lax.broadcasted_iota(jnp.int32, (512, 256), 1)
        source = row % 64 // 4 * 16 + row % 256 // 64 * 4 + row % 2 * 2 + row // 256
        one_hot = (col == source) & (row // 2 % 2 == channel)
        lefts.append(nt(one_hot.astype(F32).astype(BF16), sides[channel, 0]).astype(BF16))
    right = jnp.concatenate([sides[0, 1], sides[1, 1]], 0)
    total = nn(jnp.concatenate(lefts, 1), right)
    blocks = []
    for zl in range(2):
        lanes = slice(128 * zl, 128 * zl + 128)
        blocks.extend(halves_swapped(total[0:256, lanes], total[256:512, lanes]))
    return jnp.concatenate(
        [b[64 * zh : 64 * zh + 64] for zh in range(4) for b in blocks], 0
    ).astype(BF16)


def last_math(gathered, state, gate, out_w):
    parts = [gathered[256 * zh : 256 * zh + 256].astype(F32) for zh in range(4)]
    product = parts[0] + parts[1] + parts[2] + parts[3]
    refined = residual(
        product, lambda h: h % 32 // 2 * 8 + h // 32 * 2 + h % 2, out_w, state, gate
    )
    eye = identity(128)
    return jnp.concatenate([nt(eye, refined[0:128]), nt(eye, refined[128:256])], 0).astype(BF16)


def first_kernel(own_hbm, in_hbm, gate_hbm, sent, state, gate, own, in_w, gate_w, done):
    copies = [
        pltpu.make_async_copy(own_hbm, own, done.at[0]),
        pltpu.make_async_copy(in_hbm.at[0], in_w, done.at[1]),
        pltpu.make_async_copy(gate_hbm.at[0], gate_w, done.at[2]),
    ]
    for copy in copies:
        copy.start()
    for copy in copies:
        copy.wait()
    sent[...], state[...], gate[...] = first_math(own[...], in_w[...], gate_w[...])


def outgoing_kernel(received, partner, sent):
    sent[...] = outgoing_math(lax.axis_index("c"), received[...], partner[...])


def middle_kernel(gathered, state, gate, out_w, in_w, gate_w, sent, middle, next_gate):
    sent[...], middle[...], next_gate[...] = middle_math(
        gathered[...], state[...], gate[...], out_w[0], in_w[1], gate_w[1]
    )


def incoming_kernel(received, sent):
    sent[...] = incoming_math(received[...])


def last_kernel(gathered, state, gate, out_w, refined):
    refined[...] = last_math(gathered[...], state[...], gate[...], out_w[1])


def call(kernel, outs, *arrays, space=pltpu.VMEM, scratch=()):
    vmem = pl.BlockSpec(memory_space=pltpu.VMEM)
    return pl.pallas_call(
        kernel,
        out_shape=tuple(jax.ShapeDtypeStruct(shape, dtype) for shape, dtype in outs),
        in_specs=[pl.BlockSpec(memory_space=space)] * len(arrays),
        out_specs=tuple(vmem for _ in outs),
        scratch_shapes=scratch,
        compiler_params=pltpu.CompilerParams(vmem_limit_bytes=16 << 20),
    )(*arrays)


def exchanged(rows, axes):
    blocks = rows.reshape(lax.axis_size(axes), -1, 128)
    return lax.all_to_all(blocks, axes, 0, 0, tiled=True).reshape(rows.shape)


def from_partner(value):
    return lax.ppermute(value, "c", [(0, 1), (1, 0)])


def per_device(pair_rep, in_weights, gate_weights, out_weights):
    own = pair_rep.reshape(256, 128)
    kept = ((256, 128), F32)
    sources = [
        pltpu.with_memory_space_constraint(v, pltpu.HBM) for v in (own, in_weights, gate_weights)
    ]
    sent, state, gate = call(
        first_kernel, [((512, 128), BF16), kept, kept], *sources,
        space=pltpu.HBM,
        scratch=[
            pltpu.VMEM((256, 128), BF16), pltpu.VMEM((128, 512), BF16),
            pltpu.VMEM((128, 128), BF16), pltpu.SemaphoreType.DMA((3,)),
        ],
    )
    received = exchanged(sent, CHIPS)
    (sent,) = call(outgoing_kernel, [((256, 128), BF16)], received, from_partner(received))
    sent, state, gate = call(
        middle_kernel, [((512, 128), BF16), kept, kept],
        exchanged(sent, CHIPS), state, gate, out_weights, in_weights, gate_weights,
    )
    (sent,) = call(incoming_kernel, [((1024, 128), BF16)], exchanged(sent, LAYER))
    (refined,) = call(
        last_kernel, [((256, 128), BF16)], exchanged(sent, ALL), state, gate, out_weights
    )
    return refined.reshape(pair_rep.shape)


def solution(mesh):
    fine = Mesh(mesh.devices.reshape(4, 4, 4, 2, 2), ("y", "x", "zh", "zl", "c"))
    placed = P(("y", "x", "zh"), ("zl", "c"), None)
    return jax.shard_map(
        per_device, mesh=fine, in_specs=(placed, P(), P(), P()), out_specs=placed, check_vma=False
    )
```

```python
import jax
import jax.numpy as jnp
import numpy as np
from jax import lax
from jax.experimental import pallas as pl
from jax.experimental.pallas import tpu as pltpu
from jax.sharding import Mesh, PartitionSpec as P

EPSILON = 1e-05
BF16 = jnp.bfloat16
F32 = jnp.float32

CHIPS = ("zl", "y", "x", "zh")
TO_OWNERS = ("zl", "c", "y", "x", "zh")
LAYER = ("zl", "c", "y", "x")
FROM_LAYER = ("zh", "zl", "c", "y", "x")


def nn(a, b):
    return lax.dot_general(a, b, (((1,), (0,)), ((), ())), preferred_element_type=F32)


def nt(a, b):
    return lax.dot_general(a, b, (((1,), (1,)), ((), ())), preferred_element_type=F32)


def moved(one_hot, values):
    return nn(one_hot, values).astype(BF16)


def one_hot(rows, cols, source, valid=lambda i: i >= 0):
    index = np.arange(rows)
    hits = np.arange(cols)[None, :] == np.where(valid(index), source(index), -1)[:, None]
    return hits.astype(jnp.bfloat16)


DEAL = one_hot(256, 256, lambda i: i % 4 * 64 + i // 4)
SIDES = one_hot(256, 256, lambda i: i % 128 // 2 * 4 + i // 128 * 2 + i % 2)
ROWS = one_hot(256, 256, lambda i: i % 2 * 128 + i // 2)
TAKE = one_hot(128, 128, lambda i: i % 16 * 8 + i // 16)
TARGETS = np.stack(
    [
        one_hot(
            512, 256,
            lambda i: i % 64 // 4 * 16 + i % 256 // 64 * 4 + i % 2 * 2 + i // 256,
            lambda i: i // 2 % 2 == channel,
        )
        for channel in range(2)
    ]
)
SPREAD = np.stack(
    [one_hot(256, 128, lambda i: i // 2, lambda i: i % 2 == r).T for r in range(2)]
)
EYE = one_hot(128, 128, lambda i: i)


def normalized(values):
    tiles = values.reshape(-1, 128, 128)
    shifted = tiles - jnp.mean(tiles, axis=1, keepdims=True)
    spread = jnp.mean(shifted * shifted, axis=1, keepdims=True)
    return (shifted * lax.rsqrt(spread + EPSILON)).reshape(values.shape).astype(BF16)


def normalized_mixed(values):
    def mean(array):
        total = jnp.sum(array, axis=0)
        total = total + jnp.roll(total, 4, 0)
        return (total + jnp.roll(total, 2, 0)) / 128

    tiles = values.reshape(32, 8, 128)
    shifted = tiles - mean(tiles)
    scale = lax.rsqrt(mean(shifted * shifted) + EPSILON)
    return (shifted * scale).reshape(256, 128).astype(BF16)


def sigmoid(x):
    return 1.0 / (1.0 + jnp.exp(-x))


def halves_swapped(a, b):
    low = lax.broadcasted_iota(jnp.int32, a.shape, 1) < 64
    return jnp.where(low, a, jnp.roll(b, 64, 1)), jnp.where(low, jnp.roll(a, 64, 1), b)


def transposed(weights, eye):
    blocks = [nt(eye, weights[:, k : k + 128]) for k in range(0, weights.shape[1], 128)]
    return jnp.concatenate(blocks, 0).astype(BF16)


def sent_operands(weights, normed, deal):
    parts = []
    for r in range(2):
        projected = nn(weights, normed[128 * r : 128 * r + 128])
        for side in range(2):
            gate, value = (projected[k : k + 128] for k in (256 * side, 256 * side + 128))
            parts.append((sigmoid(gate) * value).astype(BF16))
    parts = [parts[k] for k in (0, 2, 1, 3)]
    return jnp.concatenate(
        [moved(deal, jnp.concatenate([p[k : k + 64] for p in parts], 0)) for k in (0, 64)], 0
    )


def gates(weights, state):
    normed = normalized(state)
    return jnp.concatenate([sigmoid(nn(weights, normed[k : k + 128])) for k in (0, 128)], 0)


def residual(product, spread_w, state, gate):
    update = nn(spread_w, normalized_mixed(product))
    return (state + gate * update).astype(BF16)


def first_math(own, in_w, eye, deal):
    state = jnp.concatenate([nt(eye, own[0:128]), nt(eye, own[128:256])], 0)
    return sent_operands(transposed(in_w, eye), normalized(state), deal), state


def side_math(state, in_w, gate_w, out_w, eye, spread):
    gate_t = [transposed(gate_w[u], eye) for u in range(2)]
    out_t = [transposed(out_w[u], eye) for u in range(2)]
    spread_w = [jnp.concatenate([moved(t, spread[r]) for r in range(2)], 0) for t in out_t]
    return gates(gate_t[0], state), transposed(in_w[1], eye), gate_t[1], *spread_w


def outgoing_math(received, sides, rows):
    split = [nn(sides, received[256 * zl : 256 * zl + 256]) for zl in range(2)]
    left = [v.astype(BF16) for v in halves_swapped(split[0][0:128], split[1][0:128])]
    right = jnp.concatenate(halves_swapped(split[0][128:256], split[1][128:256]), 0)
    right = moved(rows, right.astype(BF16))
    even, odd = (nt(v, right) for v in left)
    blocks = []
    for k in (0, 128):
        blocks.extend(halves_swapped(even[:, k : k + 128], odd[:, k : k + 128]))
    return jnp.concatenate(blocks, 0).astype(BF16)


def middle_math(gathered, state, gate, spread_w, in_t, deal):
    parts = gathered.astype(F32).reshape(2, 2, 128, 128)
    product = (parts[:, 0] + parts[:, 1]).reshape(256, 128)
    middle = residual(product, spread_w, state, gate).astype(F32)
    return sent_operands(in_t, normalized(middle), deal), middle


def incoming_math(received, take, targets):
    blocks = [nn(take, received[128 * ka : 128 * ka + 128]) for ka in range(4)]
    swapped = [halves_swapped(blocks[0], blocks[1]), halves_swapped(blocks[2], blocks[3])]

    def side_of(place):
        rows = slice(32 * place, 32 * place + 32)
        return jnp.concatenate(
            [jnp.concatenate([half[rows] for half in pair], 0) for pair in swapped], 1
        ).astype(BF16)

    lefts = [nt(targets[channel], side_of(2 * channel)).astype(BF16) for channel in range(2)]
    right = jnp.concatenate([side_of(1), side_of(3)], 0)
    total = nn(jnp.concatenate(lefts, 1), right)
    blocks = []
    for k in (0, 128):
        blocks.extend(halves_swapped(total[0:256, k : k + 128], total[256:512, k : k + 128]))
    return jnp.concatenate(
        [b[64 * zh : 64 * zh + 64] for zh in range(4) for b in blocks], 0
    ).astype(BF16)


def last_math(gathered, state, gate, spread_w, eye):
    product = jnp.sum(gathered.astype(F32).reshape(4, 256, 128), axis=0)
    refined = residual(product, spread_w, state, gate)
    return jnp.concatenate([nt(eye, refined[0:128]), nt(eye, refined[128:256])], 0).astype(BF16)


def first_kernel(own_hbm, in_hbm, eye_hbm, deal_hbm, sent, state, own, in_w, eye, deal, done):
    copies = [
        pltpu.make_async_copy(source, target, done.at[k])
        for k, (source, target) in enumerate(
            ((own_hbm, own), (in_hbm.at[0], in_w), (eye_hbm, eye), (deal_hbm, deal))
        )
    ]
    for copy in copies:
        copy.start()
    for copy in copies:
        copy.wait()
    sent[...], state[...] = first_math(own[...], in_w[...], eye[...], deal[...])


def side_kernel(state, in_w, gate_w, out_w, eye, spread, gate, in_t, gate_t, spread_0, spread_1):
    gate[...], in_t[...], gate_t[...], spread_0[...], spread_1[...] = side_math(
        state[...], in_w[...], gate_w[...], out_w[...], eye[...], spread[...]
    )


def outgoing_kernel(received, sides, rows, sent):
    sent[...] = outgoing_math(received[...], sides[...], rows[...])


def middle_kernel(gathered, state, gate, spread_w, in_t, deal, sent, middle):
    sent[...], middle[...] = middle_math(
        gathered[...], state[...], gate[...], spread_w[...], in_t[...], deal[...]
    )


def gate_kernel(gate_t, state, gate):
    gate[...] = gates(gate_t[...], state[...])


def incoming_kernel(received, take, targets, sent):
    sent[...] = incoming_math(received[...], take[...], targets[...])


def last_kernel(gathered, state, gate, spread_w, eye, refined):
    refined[...] = last_math(gathered[...], state[...], gate[...], spread_w[...], eye[...])


def call(kernel, outs, *arrays, space=pltpu.VMEM, scratch=()):
    vmem = pl.BlockSpec(memory_space=pltpu.VMEM)
    results = pl.pallas_call(
        kernel,
        out_shape=tuple(jax.ShapeDtypeStruct(shape, dtype) for shape, dtype in outs),
        in_specs=[pl.BlockSpec(memory_space=space)] * len(arrays),
        out_specs=tuple(vmem for _ in outs),
        scratch_shapes=scratch,
        compiler_params=pltpu.CompilerParams(vmem_limit_bytes=16 << 20),
        cost_estimate=pl.CostEstimate(flops=400_000_000, bytes_accessed=1 << 20, transcendentals=0),
    )(*arrays)
    return results if len(results) > 1 else results[0]


def exchanged(rows, axes):
    blocks = rows.reshape(lax.axis_size(axes), -1, 128)
    return lax.all_to_all(blocks, axes, 0, 0, tiled=True).reshape(rows.shape)


def per_device(pair_rep, in_weights, gate_weights, out_weights):
    eye, deal = jnp.asarray(EYE), jnp.asarray(DEAL)
    kept = ((256, 128), F32)
    wide = ((256, 256), BF16)
    inputs = [pair_rep.reshape(256, 128), in_weights, eye, deal]
    sent, state = call(
        first_kernel, [((512, 128), BF16), kept],
        *(pltpu.with_memory_space_constraint(v, pltpu.HBM) for v in inputs),
        space=pltpu.HBM,
        scratch=[
            pltpu.VMEM((256, 128), BF16), pltpu.VMEM((128, 512), BF16),
            pltpu.VMEM((128, 128), BF16), pltpu.VMEM((256, 256), BF16),
            pltpu.SemaphoreType.DMA((4,)),
        ],
    )
    gate, in_t, gate_t, spread_0, spread_1 = call(
        side_kernel, [kept, ((512, 128), BF16), ((128, 128), BF16), wide, wide],
        state, in_weights, gate_weights, out_weights, eye, jnp.asarray(SPREAD),
    )
    sent = call(
        outgoing_kernel, [((512, 128), BF16)],
        exchanged(sent, CHIPS), jnp.asarray(SIDES), jnp.asarray(ROWS),
    )
    sent, state = call(
        middle_kernel, [((512, 128), BF16), kept],
        exchanged(sent, TO_OWNERS), state, gate, spread_0, in_t, deal,
    )
    gate = call(gate_kernel, [kept], gate_t, state)
    sent = call(
        incoming_kernel, [((1024, 128), BF16)],
        exchanged(sent, LAYER), jnp.asarray(TAKE), jnp.asarray(TARGETS),
    )
    refined = call(
        last_kernel, [((256, 128), BF16)],
        exchanged(sent, FROM_LAYER), state, gate, spread_1, eye,
    )
    return refined.reshape(pair_rep.shape)


def solution(mesh):
    fine = Mesh(mesh.devices.reshape(4, 4, 4, 2, 2), ("y", "x", "zh", "zl", "c"))
    placed = P(("y", "x", "zh"), ("zl", "c"), None)
    return jax.shard_map(
        per_device, mesh=fine, in_specs=(placed, P(), P(), P()), out_specs=placed, check_vma=False
    )
```

```python
import jax
import jax.numpy as jnp
import numpy as np
from jax import lax
from jax.experimental import pallas as pl
from jax.experimental.pallas import tpu as pltpu
from jax.sharding import Mesh, PartitionSpec as P

EPSILON = 1e-05
BF16 = jnp.bfloat16
F32 = jnp.float32

CHIPS = ("zl", "y", "x", "zh")
TO_OWNERS = ("zl", "c", "y", "x", "zh")
LAYER = ("zl", "c", "y", "x")
FROM_LAYER = ("zh", "zl", "c", "y", "x")


def nn(a, b):
    return lax.dot_general(a, b, (((1,), (0,)), ((), ())), preferred_element_type=F32)


def nt(a, b):
    return lax.dot_general(a, b, (((1,), (1,)), ((), ())), preferred_element_type=F32)


def moved(one_hot, values):
    return nn(one_hot, values).astype(BF16)


def one_hot(rows, cols, source, valid=lambda i: i >= 0):
    index = np.arange(rows)
    hits = np.arange(cols)[None, :] == np.where(valid(index), source(index), -1)[:, None]
    return hits.astype(jnp.bfloat16)


DEAL = one_hot(256, 256, lambda i: i % 4 * 64 + i // 4)
SIDES = one_hot(256, 256, lambda i: i % 128 // 2 * 4 + i // 128 * 2 + i % 2)
ROWS = one_hot(256, 256, lambda i: i % 2 * 128 + i // 2)
TAKE = one_hot(128, 128, lambda i: i % 16 * 8 + i // 16)
TARGETS = np.stack(
    [
        one_hot(
            512, 256,
            lambda i: i % 64 // 4 * 16 + i % 256 // 64 * 4 + i % 2 * 2 + i // 256,
            lambda i: i // 2 % 2 == channel,
        )
        for channel in range(2)
    ]
)
SPREAD = np.stack(
    [one_hot(256, 128, lambda i: i // 2, lambda i: i % 2 == r).T for r in range(2)]
)


def identity():
    row = lax.broadcasted_iota(jnp.int32, (128, 128), 0)
    col = lax.broadcasted_iota(jnp.int32, (128, 128), 1)
    return (row == col).astype(F32).astype(BF16)


def normalized(values):
    tiles = values.reshape(-1, 128, 128)
    shifted = tiles - jnp.mean(tiles, axis=1, keepdims=True)
    spread = jnp.mean(shifted * shifted, axis=1, keepdims=True)
    return (shifted * lax.rsqrt(spread + EPSILON)).reshape(values.shape).astype(BF16)


def normalized_mixed(values):
    def mean(array):
        total = jnp.sum(array, axis=0)
        total = total + jnp.roll(total, 4, 0)
        return (total + jnp.roll(total, 2, 0)) / 128

    tiles = values.reshape(32, 8, 128)
    shifted = tiles - mean(tiles)
    scale = lax.rsqrt(mean(shifted * shifted) + EPSILON)
    return (shifted * scale).reshape(256, 128).astype(BF16)


def sigmoid(x):
    return 1.0 / (1.0 + jnp.exp(-x))


def halves_swapped(a, b):
    low = lax.broadcasted_iota(jnp.int32, a.shape, 1) < 64
    return jnp.where(low, a, jnp.roll(b, 64, 1)), jnp.where(low, jnp.roll(a, 64, 1), b)


def transposed(weights, eye):
    blocks = [nt(eye, weights[:, k : k + 128]) for k in range(0, weights.shape[1], 128)]
    return jnp.concatenate(blocks, 0).astype(BF16)


def sent_operands(weights, normed, deal):
    parts = []
    for r in range(2):
        projected = nn(weights, normed[128 * r : 128 * r + 128])
        for side in range(2):
            gate, value = (projected[k : k + 128] for k in (256 * side, 256 * side + 128))
            parts.append((sigmoid(gate) * value).astype(BF16))
    parts = [parts[k] for k in (0, 2, 1, 3)]
    return jnp.concatenate(
        [moved(deal, jnp.concatenate([p[k : k + 64] for p in parts], 0)) for k in (0, 64)], 0
    )


def gates(weights, state):
    normed = normalized(state)
    return jnp.concatenate([sigmoid(nn(weights, normed[k : k + 128])) for k in (0, 128)], 0)


def residual(product, spread_w, state, gate):
    update = nn(spread_w, normalized_mixed(product))
    return (state + gate * update).astype(BF16)


def first_math(own, in_w, eye, deal):
    state = jnp.concatenate([nt(eye, own[0:128]), nt(eye, own[128:256])], 0)
    return sent_operands(transposed(in_w, eye), normalized(state), deal), state


def side_math(state, in_w, gate_w, out_w, eye, spread):
    gate_t = [transposed(gate_w[u], eye) for u in range(2)]
    out_t = [transposed(out_w[u], eye) for u in range(2)]
    spread_w = [jnp.concatenate([moved(t, spread[r]) for r in range(2)], 0) for t in out_t]
    return gates(gate_t[0], state), transposed(in_w, eye), gate_t[1], *spread_w


def outgoing_math(received, sides, rows):
    split = [nn(sides, received[256 * zl : 256 * zl + 256]) for zl in range(2)]
    left = [v.astype(BF16) for v in halves_swapped(split[0][0:128], split[1][0:128])]
    right = jnp.concatenate(halves_swapped(split[0][128:256], split[1][128:256]), 0)
    right = moved(rows, right.astype(BF16))
    even, odd = (nt(v, right) for v in left)
    blocks = []
    for k in (0, 128):
        blocks.extend(halves_swapped(even[:, k : k + 128], odd[:, k : k + 128]))
    return jnp.concatenate(blocks, 0).astype(BF16)


def middle_math(gathered, state, gate, spread_w, in_t, deal):
    parts = gathered.astype(F32).reshape(2, 2, 128, 128)
    product = (parts[:, 0] + parts[:, 1]).reshape(256, 128)
    middle = residual(product, spread_w, state, gate).astype(F32)
    return sent_operands(in_t, normalized(middle), deal), middle


def incoming_math(received, take, targets):
    blocks = [nn(take, received[128 * ka : 128 * ka + 128]) for ka in range(4)]
    swapped = [halves_swapped(blocks[0], blocks[1]), halves_swapped(blocks[2], blocks[3])]

    def side_of(place):
        rows = slice(32 * place, 32 * place + 32)
        return jnp.concatenate(
            [jnp.concatenate([half[rows] for half in pair], 0) for pair in swapped], 1
        ).astype(BF16)

    lefts = [nt(targets[channel], side_of(2 * channel)).astype(BF16) for channel in range(2)]
    right = jnp.concatenate([side_of(1), side_of(3)], 0)
    total = nn(jnp.concatenate(lefts, 1), right)
    blocks = []
    for k in (0, 128):
        blocks.extend(halves_swapped(total[0:256, k : k + 128], total[256:512, k : k + 128]))
    return jnp.concatenate(
        [b[64 * zh : 64 * zh + 64] for zh in range(4) for b in blocks], 0
    ).astype(BF16)


def last_math(gathered, state, gate, spread_w, eye):
    product = jnp.sum(gathered.astype(F32).reshape(4, 256, 128), axis=0)
    refined = residual(product, spread_w, state, gate)
    return jnp.concatenate([nt(eye, refined[0:128]), nt(eye, refined[128:256])], 0).astype(BF16)


def first_kernel(
    own_hbm, in_hbm, deal_hbm, gate_hbm, out_hbm,
    sent, state, next_in, gate_w, out_w, own, in_w, deal, done,
):
    routes = (
        (own_hbm, own), (in_hbm.at[0], in_w), (deal_hbm, deal),
        (in_hbm.at[1], next_in), (gate_hbm, gate_w), (out_hbm, out_w),
    )
    copies = [
        pltpu.make_async_copy(source, target, done.at[k])
        for k, (source, target) in enumerate(routes)
    ]
    for copy in copies:
        copy.start()
    for copy in copies[:3]:
        copy.wait()
    sent[...], state[...] = first_math(own[...], in_w[...], identity(), deal[...])
    for copy in copies[3:]:
        copy.wait()


def outgoing_kernel(
    received, state, in_w, gate_w, out_w, moves, sent, gate, in_t, gate_t, spread_0, spread_1
):
    sent[...] = outgoing_math(received[...], moves[0:256], moves[256:512])
    gate[...], in_t[...], gate_t[...], spread_0[...], spread_1[...] = side_math(
        state[...], in_w[...], gate_w[...], out_w[...], identity(),
        (moves[512:640], moves[640:768]),
    )


def middle_kernel(gathered, state, gate, spread_w, in_t, deal, sent, middle):
    sent[...], middle[...] = middle_math(
        gathered[...], state[...], gate[...], spread_w[...], in_t[...], deal[...]
    )


def incoming_kernel(received, state, gate_t, take, targets, sent, gate):
    sent[...] = incoming_math(received[...], take[...], targets[...])
    gate[...] = gates(gate_t[...], state[...])


def last_kernel(gathered, state, gate, spread_w, refined):
    refined[...] = last_math(gathered[...], state[...], gate[...], spread_w[...], identity())


def call(kernel, outs, *arrays, space=pltpu.VMEM, scratch=()):
    vmem = pl.BlockSpec(memory_space=pltpu.VMEM)
    results = pl.pallas_call(
        kernel,
        out_shape=tuple(jax.ShapeDtypeStruct(shape, dtype) for shape, dtype in outs),
        in_specs=[pl.BlockSpec(memory_space=space)] * len(arrays),
        out_specs=tuple(vmem for _ in outs),
        scratch_shapes=scratch,
        compiler_params=pltpu.CompilerParams(vmem_limit_bytes=16 << 20),
    )(*arrays)
    return results if len(results) > 1 else results[0]


def exchanged(rows, axes):
    blocks = rows.reshape(lax.axis_size(axes), -1, 128)
    return lax.all_to_all(blocks, axes, 0, 0, tiled=True).reshape(rows.shape)


def per_device(pair_rep, in_weights, gate_weights, out_weights):
    deal = jnp.asarray(DEAL)
    kept = ((256, 128), F32)
    wide = ((256, 256), BF16)
    inputs = [pair_rep.reshape(256, 128), in_weights, deal, gate_weights, out_weights]
    squares = ((2, 128, 128), BF16)
    sent, state, next_in, gate_w, out_w = call(
        first_kernel, [((512, 128), BF16), kept, ((128, 512), BF16), squares, squares],
        *(pltpu.with_memory_space_constraint(v, pltpu.HBM) for v in inputs),
        space=pltpu.HBM,
        scratch=[
            pltpu.VMEM((256, 128), BF16), pltpu.VMEM((128, 512), BF16),
            pltpu.VMEM((256, 256), BF16), pltpu.SemaphoreType.DMA((6,)),
        ],
    )
    sent, gate, in_t, gate_t, spread_0, spread_1 = call(
        outgoing_kernel,
        [((512, 128), BF16), kept, ((512, 128), BF16), ((128, 128), BF16), wide, wide],
        exchanged(sent, CHIPS), state, next_in, gate_w, out_w,
        jnp.asarray(np.concatenate([SIDES, ROWS, *SPREAD], 0)),
    )
    sent, state = call(
        middle_kernel, [((512, 128), BF16), kept],
        exchanged(sent, TO_OWNERS), state, gate, spread_0, in_t, deal,
    )
    sent, gate = call(
        incoming_kernel, [((1024, 128), BF16), kept],
        exchanged(sent, LAYER), state, gate_t, jnp.asarray(TAKE), jnp.asarray(TARGETS),
    )
    refined = call(
        last_kernel, [((256, 128), BF16)],
        exchanged(sent, FROM_LAYER), state, gate, spread_1,
    )
    return refined.reshape(pair_rep.shape)


def solution(mesh):
    fine = Mesh(mesh.devices.reshape(4, 4, 4, 2, 2), ("y", "x", "zh", "zl", "c"))
    placed = P(("y", "x", "zh"), ("zl", "c"), None)
    return jax.shard_map(
        per_device, mesh=fine, in_specs=(placed, P(), P(), P()), out_specs=placed, check_vma=False
    )
```

```python
import jax
import jax.numpy as jnp
import numpy as np
from jax import lax
from jax.experimental import pallas as pl
from jax.experimental.pallas import tpu as pltpu
from jax.sharding import Mesh, PartitionSpec as P

EPSILON = 1e-05
BF16 = jnp.bfloat16
F32 = jnp.float32

CHIPS = ("zl", "y", "x", "zh")
TO_OWNERS = ("zl", "c", "y", "x", "zh")
LAYER = ("c", "zl", "y", "x")
FROM_LAYER = ("zh", "zl", "y", "x")


def nn(a, b):
    return lax.dot_general(a, b, (((1,), (0,)), ((), ())), preferred_element_type=F32)


def nt(a, b):
    return lax.dot_general(a, b, (((1,), (1,)), ((), ())), preferred_element_type=F32)


def moved(one_hot, values):
    return nn(one_hot, values).astype(BF16)


def moved_t(one_hot, values):
    return nt(one_hot, values).astype(BF16)


def one_hot(rows, cols, source, valid=lambda i: i >= 0):
    index = np.arange(rows)
    hits = np.arange(cols)[None, :] == np.where(valid(index), source(index), -1)[:, None]
    return hits.astype(jnp.bfloat16)


DEAL = one_hot(256, 256, lambda i: i % 4 * 64 + i // 4)
SIDES = one_hot(256, 256, lambda i: i % 128 // 2 * 4 + i // 128 * 2 + i % 2)
ROWS = one_hot(256, 256, lambda i: i % 2 * 128 + i // 2)
TAKE = np.concatenate(
    [
        one_hot(
            128, 256,
            lambda i: i % 16 * 16 + i // 32 * 4 + side * 2 + i // 16 % 2,
        )
        for side in range(2)
    ]
)
TARGETS = one_hot(
    256, 256, lambda i: i % 32 // 2 * 16 + i % 128 // 32 * 4 + i % 2 * 2 + i // 128
)
MIX = one_hot(128, 128, lambda i: i % 8 // 2 * 32 + i // 8 * 2 + i % 2)
SPREAD = np.stack(
    [one_hot(256, 128, lambda i: i // 2, lambda i: i % 2 == r).T for r in range(2)]
)


def identity():
    row = lax.broadcasted_iota(jnp.int32, (128, 128), 0)
    col = lax.broadcasted_iota(jnp.int32, (128, 128), 1)
    return (row == col).astype(F32).astype(BF16)


def normalized(values):
    tiles = values.reshape(-1, 128, 128)
    shifted = tiles - jnp.mean(tiles, axis=1, keepdims=True)
    spread = jnp.mean(shifted * shifted, axis=1, keepdims=True)
    return (shifted * lax.rsqrt(spread + EPSILON)).reshape(values.shape).astype(BF16)


def normalized_mixed(values):
    def mean(array):
        total = jnp.sum(array, axis=0)
        total = total + jnp.roll(total, 4, 0)
        return (total + jnp.roll(total, 2, 0)) / 128

    tiles = values.reshape(32, 8, 128)
    shifted = tiles - mean(tiles)
    scale = lax.rsqrt(mean(shifted * shifted) + EPSILON)
    return (shifted * scale).reshape(256, 128).astype(BF16)


def sigmoid(x):
    return 1.0 / (1.0 + jnp.exp(-x))


def halves_swapped(a, b):
    low = lax.broadcasted_iota(jnp.int32, a.shape, 1) < 64
    return jnp.where(low, a, jnp.roll(b, 64, 1)), jnp.where(low, jnp.roll(a, 64, 1), b)


def transposed(weights, eye):
    blocks = [nt(eye, weights[:, k : k + 128]) for k in range(0, weights.shape[1], 128)]
    return jnp.concatenate(blocks, 0).astype(BF16)


def sent_operands(weights, normed, deal):
    parts = []
    for r in range(2):
        projected = nn(weights, normed[128 * r : 128 * r + 128])
        for side in range(2):
            gate, value = (projected[k : k + 128] for k in (256 * side, 256 * side + 128))
            parts.append((sigmoid(gate) * value).astype(BF16))
    parts = [parts[k] for k in (0, 2, 1, 3)]
    return jnp.concatenate(
        [moved(deal, jnp.concatenate([p[k : k + 64] for p in parts], 0)) for k in (0, 64)], 0
    )


def gates(weights, state):
    normed = normalized(state)
    return jnp.concatenate([sigmoid(nn(weights, normed[k : k + 128])) for k in (0, 128)], 0)


def residual(product, spread_w, state, gate):
    update = nn(spread_w, normalized_mixed(product))
    return (state + gate * update).astype(BF16)


def first_math(own, in_w, deal):
    values = own.astype(F32)
    shifted = values - jnp.mean(values, axis=1, keepdims=True)
    spread = jnp.mean(shifted * shifted, axis=1, keepdims=True)
    normed = (shifted * lax.rsqrt(spread + EPSILON)).astype(BF16)
    projected = nn(normed, in_w)
    blocks = ([], [])
    for k in (0, 256):
        product = sigmoid(projected[:, k : k + 128]) * projected[:, k + 128 : k + 256]
        for block, half in zip(blocks, halves_swapped(product[0:128], product[128:256])):
            block.append(half)
    return jnp.concatenate(
        [moved_t(deal, jnp.concatenate(b, 1).astype(BF16)) for b in blocks], 0
    )


def side_math(own, in_w, gate_w, out_w, eye, spread):
    state = jnp.concatenate([nt(eye, own[0:128]), nt(eye, own[128:256])], 0)
    gate_t = [transposed(gate_w[u], eye) for u in range(2)]
    out_t = [transposed(out_w[u], eye) for u in range(2)]
    spread_w = [jnp.concatenate([moved(t, spread[r]) for r in range(2)], 0) for t in out_t]
    return state, gates(gate_t[0], state), transposed(in_w, eye), gate_t[1], *spread_w


def outgoing_math(received, sides, rows):
    split = [nn(sides, received[256 * zl : 256 * zl + 256]) for zl in range(2)]
    left = [v.astype(BF16) for v in halves_swapped(split[0][0:128], split[1][0:128])]
    right = jnp.concatenate(halves_swapped(split[0][128:256], split[1][128:256]), 0)
    right = moved(rows, right.astype(BF16))
    even, odd = (nt(v, right) for v in left)
    blocks = []
    for k in (0, 128):
        blocks.extend(halves_swapped(even[:, k : k + 128], odd[:, k : k + 128]))
    return jnp.concatenate(blocks, 0).astype(BF16)


def middle_math(gathered, state, gate, spread_w, in_t, deal):
    parts = gathered.astype(F32).reshape(2, 2, 128, 128)
    product = (parts[:, 0] + parts[:, 1]).reshape(256, 128)
    middle = residual(product, spread_w, state, gate).astype(F32)
    sent = sent_operands(in_t, normalized(middle), deal)
    return jnp.concatenate([sent, sent], 0), middle


def incoming_math(received, own_core, take, targets, mix):
    blocks = [nn(take[0:128], received[256 * k : 256 * k + 256]) for k in range(4)]
    lefts = [halves_swapped(blocks[zl], blocks[zl + 2]) for zl in range(2)]
    blocks = [nn(take[128:256], own_core[256 * zl : 256 * zl + 256]) for zl in range(2)]
    rights = halves_swapped(*blocks)
    totals = []
    for channel in range(4):
        rows = slice(32 * channel, 32 * channel + 32)
        left = jnp.concatenate(
            [jnp.concatenate([half[rows] for half in pair], 0) for pair in lefts], 1
        )
        right = jnp.concatenate([half[rows] for half in rights], 0)
        total = nn(moved_t(targets, left.astype(BF16)), right.astype(BF16))
        totals.append([v.astype(BF16) for v in halves_swapped(total[0:128], total[128:256])])
    sent = []
    for zh in range(4):
        rows = slice(32 * zh, 32 * zh + 32)
        for zl in range(2):
            sent.append(moved(mix, jnp.concatenate([pair[zl][rows] for pair in totals], 0)))
    return jnp.concatenate(sent, 0)


def last_math(gathered, state, gate, spread_w, eye):
    product = jnp.sum(gathered.astype(F32).reshape(4, 256, 128), axis=0)
    refined = residual(product, spread_w, state, gate)
    return jnp.concatenate([nt(eye, refined[0:128]), nt(eye, refined[128:256])], 0).astype(BF16)


def first_kernel(
    own_hbm, in_hbm, deal_hbm, gate_hbm, out_hbm,
    sent, own, next_in, gate_w, out_w, in_w, deal, done,
):
    routes = (
        (own_hbm, own), (in_hbm.at[0], in_w), (deal_hbm, deal),
        (in_hbm.at[1], next_in), (gate_hbm, gate_w), (out_hbm, out_w),
    )
    copies = [
        pltpu.make_async_copy(source, target, done.at[k])
        for k, (source, target) in enumerate(routes)
    ]
    for copy in copies:
        copy.start()
    for copy in copies[:3]:
        copy.wait()
    sent[...] = first_math(own[...], in_w[...], deal[...])
    for copy in copies[3:]:
        copy.wait()


def outgoing_kernel(
    received, own, in_w, gate_w, out_w, moves,
    sent, state, gate, in_t, gate_t, spread_0, spread_1,
):
    sent[...] = outgoing_math(received[...], moves[0:256], moves[256:512])
    state[...], gate[...], in_t[...], gate_t[...], spread_0[...], spread_1[...] = side_math(
        own[...], in_w[...], gate_w[...], out_w[...], identity(),
        (moves[512:640], moves[640:768]),
    )


def middle_kernel(gathered, state, gate, spread_w, in_t, deal, sent, middle):
    sent[...], middle[...] = middle_math(
        gathered[...], state[...], gate[...], spread_w[...], in_t[...], deal[...]
    )


def incoming_kernel(received, state, gate_t, moves, mix, sent, gate):
    own_core = received[pl.ds(pl.multiple_of(lax.axis_index("c") * 512, 512), 512)]
    sent[...] = incoming_math(received[...], own_core, moves[0:256], moves[256:512], mix[...])
    gate[...] = gates(gate_t[...], state[...])


def last_kernel(gathered, state, gate, spread_w, refined):
    refined[...] = last_math(gathered[...], state[...], gate[...], spread_w[...], identity())


def call(kernel, outs, *arrays, space=pltpu.VMEM, scratch=()):
    vmem = pl.BlockSpec(memory_space=pltpu.VMEM)
    results = pl.pallas_call(
        kernel,
        out_shape=tuple(jax.ShapeDtypeStruct(shape, dtype) for shape, dtype in outs),
        in_specs=[pl.BlockSpec(memory_space=space)] * len(arrays),
        out_specs=tuple(vmem for _ in outs),
        scratch_shapes=scratch,
        compiler_params=pltpu.CompilerParams(vmem_limit_bytes=16 << 20),
    )(*arrays)
    return results if len(results) > 1 else results[0]


def exchanged(rows, axes):
    blocks = rows.reshape(lax.axis_size(axes), -1, 128)
    return lax.all_to_all(blocks, axes, 0, 0, tiled=True).reshape(rows.shape)


def per_device(pair_rep, in_weights, gate_weights, out_weights):
    deal = jnp.asarray(DEAL)
    kept = ((256, 128), F32)
    wide = ((256, 256), BF16)
    inputs = [pair_rep.reshape(256, 128), in_weights, deal, gate_weights, out_weights]
    block, weights, square = ((256, 128), BF16), ((128, 512), BF16), ((2, 128, 128), BF16)
    sent, own, next_in, gate_w, out_w = call(
        first_kernel, [((512, 128), BF16), block, weights, square, square],
        *(pltpu.with_memory_space_constraint(v, pltpu.HBM) for v in inputs),
        space=pltpu.HBM,
        scratch=[
            pltpu.VMEM((128, 512), BF16), pltpu.VMEM((256, 256), BF16),
            pltpu.SemaphoreType.DMA((6,)),
        ],
    )
    sent, state, gate, in_t, gate_t, spread_0, spread_1 = call(
        outgoing_kernel,
        [((512, 128), BF16), kept, kept, ((512, 128), BF16), ((128, 128), BF16), wide, wide],
        exchanged(sent, CHIPS), own, next_in, gate_w, out_w,
        jnp.asarray(np.concatenate([SIDES, ROWS, *SPREAD], 0)),
    )
    sent, state = call(
        middle_kernel, [((1024, 128), BF16), kept],
        exchanged(sent, TO_OWNERS), state, gate, spread_0, in_t, deal,
    )
    sent, gate = call(
        incoming_kernel, [((1024, 128), BF16), kept],
        exchanged(sent, LAYER), state, gate_t,
        jnp.asarray(np.concatenate([TAKE, TARGETS], 0)), jnp.asarray(MIX),
    )
    refined = call(
        last_kernel, [((256, 128), BF16)],
        exchanged(sent, FROM_LAYER), state, gate, spread_1,
    )
    return refined.reshape(pair_rep.shape)


def solution(mesh):
    fine = Mesh(mesh.devices.reshape(4, 4, 4, 2, 2), ("y", "x", "zh", "zl", "c"))
    placed = P(("y", "x", "zh"), ("zl", "c"), None)
    return jax.shard_map(
        per_device, mesh=fine, in_specs=(placed, P(), P(), P()), out_specs=placed, check_vma=False
    )
```

```python
import jax
import jax.numpy as jnp
import numpy as np
from jax import lax
from jax.experimental import pallas as pl
from jax.experimental.pallas import tpu as pltpu
from jax.sharding import Mesh, PartitionSpec as P

EPSILON = 1e-05
BF16 = jnp.bfloat16
F32 = jnp.float32

CHIPS = ("zh", "zl", "y", "x")
LAYER = ("zl", "c", "y", "x")
ALL = ("zh", "zl", "c", "y", "x")


def nn(a, b):
    return lax.dot_general(a, b, (((1,), (0,)), ((), ())), preferred_element_type=F32)


def nt(a, b):
    return lax.dot_general(a, b, (((1,), (1,)), ((), ())), preferred_element_type=F32)


def moved(one_hot, values):
    return nn(one_hot, values).astype(BF16)


def one_hot(rows, cols, source, valid=lambda i: i >= 0):
    index = np.arange(rows)
    hits = np.arange(cols)[None, :] == np.where(valid(index), source(index), -1)[:, None]
    return hits.astype(jnp.bfloat16)


DEAL = one_hot(256, 256, lambda i: i % 4 * 64 + i // 4)
SIDES = one_hot(256, 256, lambda i: i % 128 // 2 * 4 + i // 128 * 2 + i % 2)
ROWS = one_hot(
    256, 256, lambda i: i % 2 * 128 + i % 16 // 4 * 32 + i // 16 * 2 + i % 4 // 2
)
TAKE = one_hot(128, 128, lambda i: i % 16 * 8 + i // 16)
TARGETS = np.stack(
    [
        one_hot(
            512, 256,
            lambda i: i % 64 // 4 * 16 + i % 256 // 64 * 4 + i % 2 * 2 + i // 256,
            lambda i: i // 2 % 2 == channel,
        )
        for channel in range(2)
    ]
)
SPREAD = np.stack(
    [one_hot(256, 128, lambda i: i // 2, lambda i: i % 2 == r).T for r in range(2)]
)


def identity():
    row = lax.broadcasted_iota(jnp.int32, (128, 128), 0)
    col = lax.broadcasted_iota(jnp.int32, (128, 128), 1)
    return (row == col).astype(F32).astype(BF16)


def normalized(values):
    tiles = values.reshape(-1, 128, 128)
    shifted = tiles - jnp.mean(tiles, axis=1, keepdims=True)
    spread = jnp.mean(shifted * shifted, axis=1, keepdims=True)
    return (shifted * lax.rsqrt(spread + EPSILON)).reshape(values.shape).astype(BF16)


def normalized_mixed(values):
    def mean(array):
        total = jnp.sum(array, axis=0)
        total = total + jnp.roll(total, 4, 0)
        return (total + jnp.roll(total, 2, 0)) / 128

    tiles = values.reshape(32, 8, 128)
    shifted = tiles - mean(tiles)
    scale = lax.rsqrt(mean(shifted * shifted) + EPSILON)
    return (shifted * scale).reshape(256, 128).astype(BF16)


def sigmoid(x):
    return 1.0 / (1.0 + jnp.exp(-x))


def halves_swapped(a, b):
    low = lax.broadcasted_iota(jnp.int32, a.shape, 1) < 64
    return jnp.where(low, a, jnp.roll(b, 64, 1)), jnp.where(low, jnp.roll(a, 64, 1), b)


def transposed(weights, eye):
    blocks = [nt(eye, weights[:, k : k + 128]) for k in range(0, weights.shape[1], 128)]
    return jnp.concatenate(blocks, 0).astype(BF16)


def sent_operands(weights, normed, deal):
    parts = []
    for r in range(2):
        projected = nn(weights, normed[128 * r : 128 * r + 128])
        for side in range(2):
            gate, value = (projected[k : k + 128] for k in (256 * side, 256 * side + 128))
            parts.append((sigmoid(gate) * value).astype(BF16))
    parts = [parts[k] for k in (0, 2, 1, 3)]
    return jnp.concatenate(
        [moved(deal, jnp.concatenate([p[k : k + 64] for p in parts], 0)) for k in (0, 64)], 0
    )


def gates(weights, state):
    normed = normalized(state)
    return jnp.concatenate([sigmoid(nn(weights, normed[k : k + 128])) for k in (0, 128)], 0)


def residual(product, spread_w, state, gate):
    update = nn(spread_w, normalized_mixed(product))
    return (state + gate * update).astype(BF16)


def first_math(own, in_w, eye, deal):
    state = jnp.concatenate([nt(eye, own[0:128]), nt(eye, own[128:256])], 0)
    return sent_operands(transposed(in_w, eye), normalized(state), deal), state


def side_math(state, in_w, gate_w, out_w, eye, spread):
    gate_t = [transposed(gate_w[u], eye) for u in range(2)]
    out_t = [transposed(out_w[u], eye) for u in range(2)]
    spread_w = [jnp.concatenate([moved(t, spread[r]) for r in range(2)], 0) for t in out_t]
    return gates(gate_t[0], state), transposed(in_w, eye), gate_t[1], *spread_w


def outgoing_math(received, sides, rows):
    split = []
    for zl in range(2):
        starts = range(64 * zl, 512, 128)
        split.append(nn(sides, jnp.concatenate([received[k : k + 64] for k in starts], 0)))
    left = [v.astype(BF16) for v in halves_swapped(split[0][0:128], split[1][0:128])]
    right = jnp.concatenate(halves_swapped(split[0][128:256], split[1][128:256]), 0)
    right = moved(rows, right.astype(BF16))
    even, odd = (nt(v, right) for v in left)
    blocks = []
    for k in (0, 128):
        blocks.extend(halves_swapped(even[:, k : k + 128], odd[:, k : k + 128]))
    return jnp.concatenate(
        [b[32 * zh : 32 * zh + 32] for zh in range(4) for b in blocks], 0
    ).astype(BF16)


def middle_math(gathered, state, gate, spread_w, in_t, deal):
    parts = gathered.astype(F32).reshape(8, 2, 32, 128)
    product = (parts[:, 0] + parts[:, 1]).reshape(256, 128)
    middle = residual(product, spread_w, state, gate).astype(F32)
    return sent_operands(in_t, normalized(middle), deal), middle


def incoming_math(received, take, targets):
    blocks = [nn(take, received[128 * ka : 128 * ka + 128]) for ka in range(4)]
    swapped = [halves_swapped(blocks[0], blocks[1]), halves_swapped(blocks[2], blocks[3])]

    def side_of(place):
        rows = slice(32 * place, 32 * place + 32)
        return jnp.concatenate(
            [jnp.concatenate([half[rows] for half in pair], 0) for pair in swapped], 1
        ).astype(BF16)

    lefts = [nt(targets[channel], side_of(2 * channel)).astype(BF16) for channel in range(2)]
    right = jnp.concatenate([side_of(1), side_of(3)], 0)
    total = nn(jnp.concatenate(lefts, 1), right)
    blocks = []
    for k in (0, 128):
        blocks.extend(halves_swapped(total[0:256, k : k + 128], total[256:512, k : k + 128]))
    return jnp.concatenate(
        [b[64 * zh : 64 * zh + 64] for zh in range(4) for b in blocks], 0
    ).astype(BF16)


def last_math(gathered, state, gate, spread_w, eye):
    product = jnp.sum(gathered.astype(F32).reshape(4, 256, 128), axis=0)
    refined = residual(product, spread_w, state, gate)
    return jnp.concatenate([nt(eye, refined[0:128]), nt(eye, refined[128:256])], 0).astype(BF16)


def first_kernel(
    own_hbm, in_hbm, gate_hbm, out_hbm, moves_hbm,
    sent, state, next_in, gate_w, out_w, moves, own, in_w, done,
):
    routes = (
        (own_hbm, own), (in_hbm.at[0], in_w), (in_hbm.at[1], next_in),
        (gate_hbm, gate_w), (out_hbm, out_w), (moves_hbm, moves),
    )
    copies = [
        pltpu.make_async_copy(source, target, done.at[k])
        for k, (source, target) in enumerate(routes)
    ]
    for copy in copies[:2]:
        copy.start()
    row = lax.broadcasted_iota(jnp.int32, (256, 256), 0)
    col = lax.broadcasted_iota(jnp.int32, (256, 256), 1)
    deal = (col == row % 4 * 64 + row // 4).astype(F32).astype(BF16)
    for copy in copies[:2]:
        copy.wait()
    for copy in copies[2:]:
        copy.start()
    sent[...], state[...] = first_math(own[...], in_w[...], identity(), deal)
    for copy in copies[2:]:
        copy.wait()


def outgoing_kernel(
    received, state, in_w, gate_w, out_w, moves, sent, gate, in_t, gate_t, spread_0, spread_1
):
    sent[...] = outgoing_math(received[...], moves[0:256], moves[256:512])
    gate[...], in_t[...], gate_t[...], spread_0[...], spread_1[...] = side_math(
        state[...], in_w[...], gate_w[...], out_w[...], identity(),
        (moves[512:640], moves[640:768]),
    )


def middle_kernel(gathered, state, gate, spread_w, in_t, deal, sent, middle):
    sent[...], middle[...] = middle_math(
        gathered[...], state[...], gate[...], spread_w[...], in_t[...], deal[...]
    )


def incoming_kernel(received, state, gate_t, take, targets, sent, gate):
    sent[...] = incoming_math(received[...], take[...], targets[...])
    gate[...] = gates(gate_t[...], state[...])


def last_kernel(gathered, state, gate, spread_w, refined):
    refined[...] = last_math(gathered[...], state[...], gate[...], spread_w[...], identity())


def call(kernel, outs, *arrays, space=pltpu.VMEM, scratch=()):
    vmem = pl.BlockSpec(memory_space=pltpu.VMEM)
    results = pl.pallas_call(
        kernel,
        out_shape=tuple(jax.ShapeDtypeStruct(shape, dtype) for shape, dtype in outs),
        in_specs=[pl.BlockSpec(memory_space=space)] * len(arrays),
        out_specs=tuple(vmem for _ in outs),
        scratch_shapes=scratch,
        compiler_params=pltpu.CompilerParams(vmem_limit_bytes=16 << 20),
    )(*arrays)
    return results if len(results) > 1 else results[0]


def exchanged(rows, axes):
    blocks = rows.reshape(lax.axis_size(axes), -1, 128)
    return lax.all_to_all(blocks, axes, 0, 0, tiled=True).reshape(rows.shape)


def per_device(pair_rep, in_weights, gate_weights, out_weights):
    deal = jnp.asarray(DEAL)
    kept = ((256, 128), F32)
    wide = ((256, 256), BF16)
    moves = jnp.asarray(np.concatenate([SIDES, ROWS, *SPREAD], 0))
    inputs = [pair_rep.reshape(256, 128), in_weights, gate_weights, out_weights, moves]
    squares = ((2, 128, 128), BF16)
    sent, state, next_in, gate_w, out_w, moves = call(
        first_kernel,
        [((512, 128), BF16), kept, ((128, 512), BF16), squares, squares, (moves.shape, BF16)],
        *(pltpu.with_memory_space_constraint(v, pltpu.HBM) for v in inputs),
        space=pltpu.HBM,
        scratch=[
            pltpu.VMEM((256, 128), BF16), pltpu.VMEM((128, 512), BF16),
            pltpu.SemaphoreType.DMA((6,)),
        ],
    )
    sent, gate, in_t, gate_t, spread_0, spread_1 = call(
        outgoing_kernel,
        [((512, 128), BF16), kept, ((512, 128), BF16), ((128, 128), BF16), wide, wide],
        exchanged(sent, CHIPS), state, next_in, gate_w, out_w, moves,
    )
    sent, state = call(
        middle_kernel, [((512, 128), BF16), kept],
        exchanged(sent, ALL), state, gate, spread_0, in_t, deal,
    )
    sent, gate = call(
        incoming_kernel, [((1024, 128), BF16), kept],
        exchanged(sent, LAYER), state, gate_t, jnp.asarray(TAKE), jnp.asarray(TARGETS),
    )
    refined = call(
        last_kernel, [((256, 128), BF16)],
        exchanged(sent, ALL), state, gate, spread_1,
    )
    return refined.reshape(pair_rep.shape)


def solution(mesh):
    fine = Mesh(mesh.devices.reshape(4, 4, 4, 2, 2), ("y", "x", "zh", "zl", "c"))
    placed = P(("y", "x", "zh"), ("zl", "c"), None)
    return jax.shard_map(
        per_device, mesh=fine, in_specs=(placed, P(), P(), P()), out_specs=placed, check_vma=False
    )
```

```python
import jax
import jax.numpy as jnp
import numpy as np
from jax import lax
from jax.experimental import pallas as pl
from jax.experimental.pallas import tpu as pltpu
from jax.sharding import Mesh, PartitionSpec as P

EPSILON = 1e-05
BF16 = jnp.bfloat16
F32 = jnp.float32

CHIPS = ("zl", "y", "x", "zh")
TO_OWNERS = ("zl", "c", "y", "x", "zh")
LAYER = ("zl", "c", "y", "x")
FROM_LAYER = ("zh", "zl", "c", "y", "x")


def nn(a, b):
    return lax.dot_general(a, b, (((1,), (0,)), ((), ())), preferred_element_type=F32)


def nt(a, b):
    return lax.dot_general(a, b, (((1,), (1,)), ((), ())), preferred_element_type=F32)


def moved(one_hot, values):
    return nn(one_hot, values).astype(BF16)


def one_hot(rows, cols, source, valid=lambda i: i >= 0):
    index = np.arange(rows)
    hits = np.arange(cols)[None, :] == np.where(valid(index), source(index), -1)[:, None]
    return hits.astype(jnp.bfloat16)


DEAL = one_hot(256, 256, lambda i: i % 4 * 64 + i // 4)
SIDES = one_hot(256, 256, lambda i: i % 128 // 2 * 4 + i // 128 * 2 + i % 2)
ROWS = one_hot(256, 256, lambda i: i % 2 * 128 + i // 2)
TAKE = one_hot(128, 128, lambda i: i % 16 * 8 + i // 16)
TARGETS = np.stack(
    [
        one_hot(
            512, 256,
            lambda i: i % 64 // 4 * 16 + i % 256 // 64 * 4 + i % 2 * 2 + i // 256,
            lambda i: i // 2 % 2 == channel,
        )
        for channel in range(2)
    ]
)
SPREAD = np.stack(
    [one_hot(256, 128, lambda i: i // 2, lambda i: i % 2 == r).T for r in range(2)]
)


def identity():
    row = lax.broadcasted_iota(jnp.int32, (128, 128), 0)
    col = lax.broadcasted_iota(jnp.int32, (128, 128), 1)
    return (row == col).astype(F32).astype(BF16)


def normalized(values):
    tiles = values.reshape(-1, 128, 128)
    shifted = tiles - jnp.mean(tiles, axis=1, keepdims=True)
    spread = jnp.mean(shifted * shifted, axis=1, keepdims=True)
    return (shifted * lax.rsqrt(spread + EPSILON)).reshape(values.shape).astype(BF16)


def normalized_mixed(values):
    def mean(array):
        total = jnp.sum(array, axis=0)
        total = total + jnp.roll(total, 4, 0)
        return (total + jnp.roll(total, 2, 0)) / 128

    tiles = values.reshape(32, 8, 128)
    shifted = tiles - mean(tiles)
    scale = lax.rsqrt(mean(shifted * shifted) + EPSILON)
    return (shifted * scale).reshape(256, 128).astype(BF16)


def sigmoid(x):
    return 1.0 / (1.0 + jnp.exp(-x))


def halves_swapped(a, b):
    low = lax.broadcasted_iota(jnp.int32, a.shape, 1) < 64
    return jnp.where(low, a, jnp.roll(b, 64, 1)), jnp.where(low, jnp.roll(a, 64, 1), b)


def transposed(weights, eye):
    blocks = [nt(eye, weights[:, k : k + 128]) for k in range(0, weights.shape[1], 128)]
    return jnp.concatenate(blocks, 0).astype(BF16)


def sent_operands(weights, normed, deal):
    parts = []
    for r in range(2):
        projected = nn(weights, normed[128 * r : 128 * r + 128])
        for side in range(2):
            gate, value = (projected[k : k + 128] for k in (256 * side, 256 * side + 128))
            parts.append((sigmoid(gate) * value).astype(BF16))
    parts = [parts[k] for k in (0, 2, 1, 3)]
    return jnp.concatenate(
        [moved(deal, jnp.concatenate([p[k : k + 64] for p in parts], 0)) for k in (0, 64)], 0
    )


def gates(weights, state):
    normed = normalized(state)
    return jnp.concatenate([sigmoid(nn(weights, normed[k : k + 128])) for k in (0, 128)], 0)


def residual(product, spread_w, state, gate):
    update = nn(spread_w, normalized_mixed(product))
    return (state + gate * update).astype(BF16)


def first_math(own, in_w, eye, deal):
    state = jnp.concatenate([nt(eye, own[0:128]), nt(eye, own[128:256])], 0)
    return sent_operands(transposed(in_w, eye), normalized(state), deal), state


def spread_out(weights, eye, spread):
    weights = transposed(weights, eye)
    return jnp.concatenate([moved(weights, spread[0:128]), moved(weights, spread[128:256])], 0)


def outgoing_math(received, sides, rows):
    split = [nn(sides, received[256 * zl : 256 * zl + 256]) for zl in range(2)]
    left = [v.astype(BF16) for v in halves_swapped(split[0][0:128], split[1][0:128])]
    right = jnp.concatenate(halves_swapped(split[0][128:256], split[1][128:256]), 0)
    right = moved(rows, right.astype(BF16))
    even, odd = (nt(v, right) for v in left)
    blocks = []
    for k in (0, 128):
        blocks.extend(halves_swapped(even[:, k : k + 128], odd[:, k : k + 128]))
    return jnp.concatenate(blocks, 0).astype(BF16)


def middle_math(gathered, state, gate, spread_w, in_w, deal):
    in_t = transposed(in_w, identity())
    parts = gathered.astype(F32).reshape(2, 2, 128, 128)
    product = (parts[:, 0] + parts[:, 1]).reshape(256, 128)
    middle = residual(product, spread_w, state, gate).astype(F32)
    return sent_operands(in_t, normalized(middle), deal), middle


def incoming_math(received, take, targets):
    blocks = [nn(take, received[128 * ka : 128 * ka + 128]) for ka in range(4)]
    swapped = [halves_swapped(blocks[0], blocks[1]), halves_swapped(blocks[2], blocks[3])]

    def side_of(place):
        rows = slice(32 * place, 32 * place + 32)
        return jnp.concatenate(
            [jnp.concatenate([half[rows] for half in pair], 0) for pair in swapped], 1
        ).astype(BF16)

    lefts = [nt(targets[channel], side_of(2 * channel)).astype(BF16) for channel in range(2)]
    right = jnp.concatenate([side_of(1), side_of(3)], 0)
    total = nn(jnp.concatenate(lefts, 1), right)
    blocks = []
    for k in (0, 128):
        blocks.extend(halves_swapped(total[0:256, k : k + 128], total[256:512, k : k + 128]))
    return jnp.concatenate(
        [b[64 * zh : 64 * zh + 64] for zh in range(4) for b in blocks], 0
    ).astype(BF16)


def last_math(gathered, state, gate, spread_w, eye):
    product = jnp.sum(gathered.astype(F32).reshape(4, 256, 128), axis=0)
    refined = residual(product, spread_w, state, gate)
    return jnp.concatenate([nt(eye, refined[0:128]), nt(eye, refined[128:256])], 0).astype(BF16)


def first_kernel(
    own_hbm, in_hbm, gate_hbm, out_hbm, sent, state, next_in, gate_w, out_w, own, in_w, done
):
    routes = (
        (own_hbm, own), (in_hbm.at[0], in_w),
        (in_hbm.at[1], next_in), (gate_hbm, gate_w), (out_hbm, out_w),
    )
    copies = [
        pltpu.make_async_copy(source, target, done.at[k])
        for k, (source, target) in enumerate(routes)
    ]
    for copy in copies:
        copy.start()
    row = lax.broadcasted_iota(jnp.int32, (256, 256), 0)
    col = lax.broadcasted_iota(jnp.int32, (256, 256), 1)
    deal = (col == row % 4 * 64 + row // 4).astype(F32).astype(BF16)
    for copy in copies[:2]:
        copy.wait()
    sent[...], state[...] = first_math(own[...], in_w[...], identity(), deal)
    for copy in copies[2:]:
        copy.wait()


def outgoing_kernel(received, state, gate_w, out_w, moves, sent, gate, spread_w):
    eye = identity()
    sent[...] = outgoing_math(received[...], moves[0:256], moves[256:512])
    gate[...] = gates(transposed(gate_w[0], eye), state[...])
    spread_w[...] = spread_out(out_w[0], eye, moves[512:768])


def middle_kernel(gathered, state, gate, spread_w, in_w, deal, sent, middle):
    sent[...], middle[...] = middle_math(
        gathered[...], state[...], gate[...], spread_w[...], in_w[...], deal[...]
    )


def incoming_kernel(
    received, state, gate_w, out_w, take, targets, moves, sent, gate, spread_w
):
    eye = identity()
    sent[...] = incoming_math(received[...], take[...], targets[...])
    gate[...] = gates(transposed(gate_w[1], eye), state[...])
    spread_w[...] = spread_out(out_w[1], eye, moves[512:768])


def last_kernel(gathered, state, gate, spread_w, refined):
    refined[...] = last_math(gathered[...], state[...], gate[...], spread_w[...], identity())


def call(kernel, outs, *arrays, space=pltpu.VMEM, scratch=()):
    vmem = pl.BlockSpec(memory_space=pltpu.VMEM)
    results = pl.pallas_call(
        kernel,
        out_shape=tuple(jax.ShapeDtypeStruct(shape, dtype) for shape, dtype in outs),
        in_specs=[pl.BlockSpec(memory_space=space)] * len(arrays),
        out_specs=tuple(vmem for _ in outs),
        scratch_shapes=scratch,
        compiler_params=pltpu.CompilerParams(vmem_limit_bytes=16 << 20),
    )(*arrays)
    return results if len(results) > 1 else results[0]


def exchanged(rows, axes):
    blocks = rows.reshape(lax.axis_size(axes), -1, 128)
    return lax.all_to_all(blocks, axes, 0, 0, tiled=True).reshape(rows.shape)


def per_device(pair_rep, in_weights, gate_weights, out_weights):
    deal = jnp.asarray(DEAL)
    kept = ((256, 128), F32)
    wide = ((256, 256), BF16)
    moves = jnp.asarray(np.concatenate([SIDES, ROWS, *SPREAD], 0))
    inputs = [pair_rep.reshape(256, 128), in_weights, gate_weights, out_weights]
    squares = ((2, 128, 128), BF16)
    sent, state, next_in, gate_w, out_w = call(
        first_kernel, [((512, 128), BF16), kept, ((128, 512), BF16), squares, squares],
        *(pltpu.with_memory_space_constraint(v, pltpu.HBM) for v in inputs),
        space=pltpu.HBM,
        scratch=[
            pltpu.VMEM((256, 128), BF16), pltpu.VMEM((128, 512), BF16),
            pltpu.SemaphoreType.DMA((5,)),
        ],
    )
    sent, gate, spread_w = call(
        outgoing_kernel, [((512, 128), BF16), kept, wide],
        exchanged(sent, CHIPS), state, gate_w, out_w, moves,
    )
    sent, state = call(
        middle_kernel, [((512, 128), BF16), kept],
        exchanged(sent, TO_OWNERS), state, gate, spread_w, next_in, deal,
    )
    sent, gate, spread_w = call(
        incoming_kernel, [((1024, 128), BF16), kept, wide],
        exchanged(sent, LAYER), state, gate_w, out_w,
        jnp.asarray(TAKE), jnp.asarray(TARGETS), moves,
    )
    refined = call(
        last_kernel, [((256, 128), BF16)],
        exchanged(sent, FROM_LAYER), state, gate, spread_w,
    )
    return refined.reshape(pair_rep.shape)


def solution(mesh):
    fine = Mesh(mesh.devices.reshape(4, 4, 4, 2, 2), ("y", "x", "zh", "zl", "c"))
    placed = P(("y", "x", "zh"), ("zl", "c"), None)
    return jax.shard_map(
        per_device, mesh=fine, in_specs=(placed, P(), P(), P()), out_specs=placed, check_vma=False
    )
```

```python
import jax
import jax.numpy as jnp
import numpy as np
from jax import lax
from jax.experimental import pallas as pl
from jax.experimental.pallas import tpu as pltpu
from jax.sharding import Mesh, PartitionSpec as P

EPSILON = 1e-05
BF16 = jnp.bfloat16
F32 = jnp.float32

CHIPS = ("zl", "y", "x", "zh")
TO_OWNERS = ("zl", "c", "y", "x", "zh")
LAYER = ("zl", "c", "y", "x")
FROM_LAYER = ("zh", "zl", "c", "y", "x")


def nn(a, b):
    return lax.dot_general(a, b, (((1,), (0,)), ((), ())), preferred_element_type=F32)


def nt(a, b):
    return lax.dot_general(a, b, (((1,), (1,)), ((), ())), preferred_element_type=F32)


def moved(one_hot, values):
    return nn(one_hot, values).astype(BF16)


def one_hot(rows, cols, source, valid=lambda i: i >= 0):
    index = np.arange(rows)
    hits = np.arange(cols)[None, :] == np.where(valid(index), source(index), -1)[:, None]
    return hits.astype(jnp.bfloat16)


DEAL = one_hot(256, 256, lambda i: i % 4 * 64 + i // 4)
SIDES = one_hot(256, 256, lambda i: i % 128 // 2 * 4 + i // 128 * 2 + i % 2)
ROWS = one_hot(256, 256, lambda i: i % 2 * 128 + i // 2)
TAKE = one_hot(128, 128, lambda i: i % 16 * 8 + i // 16)
TARGETS = np.stack(
    [
        one_hot(
            512, 256,
            lambda i: i % 64 // 4 * 16 + i % 256 // 64 * 4 + i % 2 * 2 + i // 256,
            lambda i: i // 2 % 2 == channel,
        )
        for channel in range(2)
    ]
)
SPREAD = np.stack(
    [one_hot(256, 128, lambda i: i // 2, lambda i: i % 2 == r).T for r in range(2)]
)


def identity():
    row = lax.broadcasted_iota(jnp.int32, (128, 128), 0)
    col = lax.broadcasted_iota(jnp.int32, (128, 128), 1)
    return (row == col).astype(F32).astype(BF16)


def normalized(values):
    tiles = values.reshape(-1, 128, 128)
    shifted = tiles - jnp.mean(tiles, axis=1, keepdims=True)
    spread = jnp.mean(shifted * shifted, axis=1, keepdims=True)
    return (shifted * lax.rsqrt(spread + EPSILON)).reshape(values.shape).astype(BF16)


def normalized_mixed(values):
    def mean(array):
        total = jnp.sum(array, axis=0)
        total = total + jnp.roll(total, 4, 0)
        return (total + jnp.roll(total, 2, 0)) / 128

    tiles = values.reshape(32, 8, 128)
    shifted = tiles - mean(tiles)
    scale = lax.rsqrt(mean(shifted * shifted) + EPSILON)
    return (shifted * scale).reshape(256, 128).astype(BF16)


def sigmoid(x):
    return 1.0 / (1.0 + jnp.exp(-x))


def halves_swapped(a, b):
    low = lax.broadcasted_iota(jnp.int32, a.shape, 1) < 64
    return jnp.where(low, a, jnp.roll(b, 64, 1)), jnp.where(low, jnp.roll(a, 64, 1), b)


def transposed(weights, eye):
    blocks = [nt(eye, weights[:, k : k + 128]) for k in range(0, weights.shape[1], 128)]
    return jnp.concatenate(blocks, 0).astype(BF16)


def sent_operands(weights, normed, deal):
    parts = []
    for r in range(2):
        projected = nn(weights, normed[128 * r : 128 * r + 128])
        for side in range(2):
            gate, value = (projected[k : k + 128] for k in (256 * side, 256 * side + 128))
            parts.append((sigmoid(gate) * value).astype(BF16))
    parts = [parts[k] for k in (0, 2, 1, 3)]
    return jnp.concatenate(
        [moved(deal, jnp.concatenate([p[k : k + 64] for p in parts], 0)) for k in (0, 64)], 0
    )


def gates(weights, state):
    normed = normalized(state)
    return jnp.concatenate([sigmoid(nn(weights, normed[k : k + 128])) for k in (0, 128)], 0)


def residual(product, spread_w, state, gate):
    update = nn(spread_w, normalized_mixed(product))
    return (state + gate * update).astype(BF16)


def first_math(own, in_w, eye, deal):
    state = jnp.concatenate([nt(eye, own[0:128]), nt(eye, own[128:256])], 0)
    return sent_operands(transposed(in_w, eye), normalized(state), deal), state


def spread_out(weights, eye, spread):
    weights = transposed(weights, eye)
    return jnp.concatenate([moved(weights, spread[0:128]), moved(weights, spread[128:256])], 0)


def outgoing_math(received, sides, rows):
    split = [nn(sides, received[256 * zl : 256 * zl + 256]) for zl in range(2)]
    left = [v.astype(BF16) for v in halves_swapped(split[0][0:128], split[1][0:128])]
    right = jnp.concatenate(halves_swapped(split[0][128:256], split[1][128:256]), 0)
    right = moved(rows, right.astype(BF16))
    even, odd = (nt(v, right) for v in left)
    blocks = []
    for k in (0, 128):
        blocks.extend(halves_swapped(even[:, k : k + 128], odd[:, k : k + 128]))
    return jnp.concatenate(blocks, 0).astype(BF16)


def middle_math(gathered, state, gate, spread_w, in_w, gate_w, deal):
    in_t = transposed(in_w, identity())
    parts = gathered.astype(F32).reshape(2, 2, 128, 128)
    product = (parts[:, 0] + parts[:, 1]).reshape(256, 128)
    middle = residual(product, spread_w, state, gate).astype(F32)
    normed = normalized(middle)
    gate_t = transposed(gate_w, identity())
    gate = [sigmoid(nn(gate_t, normed[k : k + 128])) for k in (0, 128)]
    return sent_operands(in_t, normed, deal), middle, jnp.concatenate(gate, 0)


def incoming_math(received, take, targets):
    blocks = [nn(take, received[128 * ka : 128 * ka + 128]) for ka in range(4)]
    swapped = [halves_swapped(blocks[0], blocks[1]), halves_swapped(blocks[2], blocks[3])]

    def side_of(place):
        rows = slice(32 * place, 32 * place + 32)
        return jnp.concatenate(
            [jnp.concatenate([half[rows] for half in pair], 0) for pair in swapped], 1
        ).astype(BF16)

    lefts = [nt(targets[channel], side_of(2 * channel)).astype(BF16) for channel in range(2)]
    right = jnp.concatenate([side_of(1), side_of(3)], 0)
    total = nn(jnp.concatenate(lefts, 1), right)
    blocks = []
    for k in (0, 128):
        blocks.extend(halves_swapped(total[0:256, k : k + 128], total[256:512, k : k + 128]))
    return jnp.concatenate(
        [b[64 * zh : 64 * zh + 64] for zh in range(4) for b in blocks], 0
    ).astype(BF16)


def last_math(gathered, state, gate, spread_w, eye):
    product = jnp.sum(gathered.astype(F32).reshape(4, 256, 128), axis=0)
    refined = residual(product, spread_w, state, gate)
    return jnp.concatenate([nt(eye, refined[0:128]), nt(eye, refined[128:256])], 0).astype(BF16)


def first_kernel(
    own_hbm, in_hbm, gate_hbm, out_hbm, sent, state, next_in, gate_w, out_w, own, in_w, done
):
    routes = (
        (own_hbm, own), (in_hbm.at[0], in_w),
        (in_hbm.at[1], next_in), (gate_hbm, gate_w), (out_hbm, out_w),
    )
    copies = [
        pltpu.make_async_copy(source, target, done.at[k])
        for k, (source, target) in enumerate(routes)
    ]
    for copy in copies:
        copy.start()
    row = lax.broadcasted_iota(jnp.int32, (256, 256), 0)
    col = lax.broadcasted_iota(jnp.int32, (256, 256), 1)
    deal = (col == row % 4 * 64 + row // 4).astype(F32).astype(BF16)
    for copy in copies[:2]:
        copy.wait()
    sent[...], state[...] = first_math(own[...], in_w[...], identity(), deal)
    for copy in copies[2:]:
        copy.wait()


def outgoing_kernel(received, state, gate_w, out_w, moves, sent, gate, spread_w):
    eye = identity()
    sent[...] = outgoing_math(received[...], moves[0:256], moves[256:512])
    gate[...] = gates(transposed(gate_w[0], eye), state[...])
    spread_w[...] = spread_out(out_w[0], eye, moves[512:768])


def middle_kernel(
    gathered, state, gate, spread_w, in_w, gate_w, deal, sent, middle, next_gate
):
    sent[...], middle[...], next_gate[...] = middle_math(
        gathered[...], state[...], gate[...], spread_w[...], in_w[...], gate_w[1], deal[...]
    )


def incoming_kernel(received, out_w, take, targets, moves, sent, spread_w):
    sent[...] = incoming_math(received[...], take[...], targets[...])
    spread_w[...] = spread_out(out_w[1], identity(), moves[512:768])


def last_kernel(gathered, state, gate, spread_w, refined):
    refined[...] = last_math(gathered[...], state[...], gate[...], spread_w[...], identity())


def call(kernel, outs, *arrays, space=pltpu.VMEM, scratch=()):
    vmem = pl.BlockSpec(memory_space=pltpu.VMEM)
    results = pl.pallas_call(
        kernel,
        out_shape=tuple(jax.ShapeDtypeStruct(shape, dtype) for shape, dtype in outs),
        in_specs=[pl.BlockSpec(memory_space=space)] * len(arrays),
        out_specs=tuple(vmem for _ in outs),
        scratch_shapes=scratch,
        compiler_params=pltpu.CompilerParams(
            vmem_limit_bytes=16 << 20
        ),
    )(*arrays)
    return results if len(results) > 1 else results[0]


def exchanged(rows, axes):
    blocks = rows.reshape(lax.axis_size(axes), -1, 128)
    return lax.all_to_all(blocks, axes, 0, 0, tiled=True).reshape(rows.shape)


def per_device(pair_rep, in_weights, gate_weights, out_weights):
    deal = jnp.asarray(DEAL)
    kept = ((256, 128), F32)
    wide = ((256, 256), BF16)
    moves = jnp.asarray(np.concatenate([SIDES, ROWS, *SPREAD], 0))
    inputs = [pair_rep.reshape(256, 128), in_weights, gate_weights, out_weights]
    squares = ((2, 128, 128), BF16)
    sent, state, next_in, gate_w, out_w = call(
        first_kernel, [((512, 128), BF16), kept, ((128, 512), BF16), squares, squares],
        *(pltpu.with_memory_space_constraint(v, pltpu.HBM) for v in inputs),
        space=pltpu.HBM,
        scratch=[
            pltpu.VMEM((256, 128), BF16), pltpu.VMEM((128, 512), BF16),
            pltpu.SemaphoreType.DMA((5,)),
        ],
    )
    sent, gate, spread_w = call(
        outgoing_kernel, [((512, 128), BF16), kept, wide],
        exchanged(sent, CHIPS), state, gate_w, out_w, moves,
    )
    sent, state, gate = call(
        middle_kernel, [((512, 128), BF16), kept, kept],
        exchanged(sent, TO_OWNERS), state, gate, spread_w, next_in, gate_w, deal,
    )
    sent, spread_w = call(
        incoming_kernel, [((1024, 128), BF16), wide],
        exchanged(sent, LAYER), out_w,
        jnp.asarray(TAKE), jnp.asarray(TARGETS), moves,
    )
    refined = call(
        last_kernel, [((256, 128), BF16)],
        exchanged(sent, FROM_LAYER), state, gate, spread_w,
    )
    return refined.reshape(pair_rep.shape)


def solution(mesh):
    fine = Mesh(mesh.devices.reshape(4, 4, 4, 2, 2), ("y", "x", "zh", "zl", "c"))
    placed = P(("y", "x", "zh"), ("zl", "c"), None)
    return jax.shard_map(
        per_device, mesh=fine, in_specs=(placed, P(), P(), P()), out_specs=placed, check_vma=False
    )
```

```python
import jax
import jax.numpy as jnp
import numpy as np
from jax import lax
from jax.experimental import pallas as pl
from jax.experimental.pallas import tpu as pltpu
from jax.sharding import Mesh, PartitionSpec as P

EPSILON = 1e-05
BF16 = jnp.bfloat16
F32 = jnp.float32

CHIPS = ("zl", "y", "x", "zh")
TO_OWNERS = ("zl", "c", "y", "x", "zh")
LAYER = ("zl", "c", "y", "x")
FROM_LAYER = ("zh", "zl", "c", "y", "x")


def nn(a, b):
    return lax.dot_general(a, b, (((1,), (0,)), ((), ())), preferred_element_type=F32)


def nt(a, b):
    return lax.dot_general(a, b, (((1,), (1,)), ((), ())), preferred_element_type=F32)


def moved(one_hot, values):
    return nn(one_hot, values).astype(BF16)


def one_hot(rows, cols, source, valid=lambda i: i >= 0):
    index = np.arange(rows)
    hits = np.arange(cols)[None, :] == np.where(valid(index), source(index), -1)[:, None]
    return hits.astype(jnp.bfloat16)


DEAL = one_hot(256, 256, lambda i: i % 4 * 64 + i // 4)
SIDES = one_hot(256, 256, lambda i: i % 128 // 2 * 4 + i // 128 * 2 + i % 2)
ROWS = one_hot(256, 256, lambda i: i % 2 * 128 + i // 2)
TAKE = one_hot(128, 128, lambda i: i % 16 * 8 + i // 16)
TARGETS = np.stack(
    [
        one_hot(
            512, 256,
            lambda i: i % 64 // 4 * 16 + i % 256 // 64 * 4 + i % 2 * 2 + i // 256,
            lambda i: i // 2 % 2 == channel,
        )
        for channel in range(2)
    ]
)
SPREAD = np.stack(
    [one_hot(256, 128, lambda i: i // 2, lambda i: i % 2 == r).T for r in range(2)]
)


def identity():
    row = lax.broadcasted_iota(jnp.int32, (128, 128), 0)
    col = lax.broadcasted_iota(jnp.int32, (128, 128), 1)
    return (row == col).astype(F32).astype(BF16)


def normalized(values):
    tiles = values.reshape(-1, 128, 128)
    shifted = tiles - jnp.mean(tiles, axis=1, keepdims=True)
    spread = jnp.mean(shifted * shifted, axis=1, keepdims=True)
    return (shifted * lax.rsqrt(spread + EPSILON)).reshape(values.shape).astype(BF16)


def normalized_mixed(values):
    def mean(array):
        total = jnp.sum(array, axis=0)
        total = total + jnp.roll(total, 4, 0)
        return (total + jnp.roll(total, 2, 0)) / 128

    tiles = values.reshape(32, 8, 128)
    shifted = tiles - mean(tiles)
    scale = lax.rsqrt(mean(shifted * shifted) + EPSILON)
    return (shifted * scale).reshape(256, 128).astype(BF16)


def sigmoid(x):
    return 1.0 / (1.0 + jnp.exp(-x))


def halves_swapped(a, b):
    low = lax.broadcasted_iota(jnp.int32, a.shape, 1) < 64
    return jnp.where(low, a, jnp.roll(b, 64, 1)), jnp.where(low, jnp.roll(a, 64, 1), b)


def transposed(weights, eye):
    blocks = [nt(eye, weights[:, k : k + 128]) for k in range(0, weights.shape[1], 128)]
    return jnp.concatenate(blocks, 0).astype(BF16)


def sent_operands(weights, normed, deal):
    parts = []
    for r in range(2):
        projected = nn(weights, normed[128 * r : 128 * r + 128])
        for side in range(2):
            gate, value = (projected[k : k + 128] for k in (256 * side, 256 * side + 128))
            parts.append((sigmoid(gate) * value).astype(BF16))
    parts = [parts[k] for k in (0, 2, 1, 3)]
    return jnp.concatenate(
        [moved(deal, jnp.concatenate([p[k : k + 64] for p in parts], 0)) for k in (0, 64)], 0
    )


def gates(weights, normed):
    weights = transposed(weights, identity())
    return jnp.concatenate([sigmoid(nn(weights, normed[k : k + 128])) for k in (0, 128)], 0)


def residual(product, spread_w, state, gate):
    update = nn(spread_w, normalized_mixed(product))
    return (state + gate * update).astype(BF16)


def first_math(own, in_w, gate_w, eye, deal):
    state = jnp.concatenate([nt(eye, own[0:128]), nt(eye, own[128:256])], 0)
    normed = normalized(state)
    return sent_operands(transposed(in_w, eye), normed, deal), state, gates(gate_w, normed)


def spread_out(weights, eye, spread):
    weights = transposed(weights, eye)
    return jnp.concatenate([moved(weights, spread[0:128]), moved(weights, spread[128:256])], 0)


def outgoing_math(received, sides, rows):
    split = [nn(sides, received[256 * zl : 256 * zl + 256]) for zl in range(2)]
    left = [v.astype(BF16) for v in halves_swapped(split[0][0:128], split[1][0:128])]
    right = jnp.concatenate(halves_swapped(split[0][128:256], split[1][128:256]), 0)
    right = moved(rows, right.astype(BF16))
    even, odd = (nt(v, right) for v in left)
    blocks = []
    for k in (0, 128):
        blocks.extend(halves_swapped(even[:, k : k + 128], odd[:, k : k + 128]))
    return jnp.concatenate(blocks, 0).astype(BF16)


def middle_math(gathered, state, gate, spread_w, in_w, gate_w, deal):
    in_t = transposed(in_w, identity())
    parts = gathered.astype(F32).reshape(2, 2, 128, 128)
    product = (parts[:, 0] + parts[:, 1]).reshape(256, 128)
    middle = residual(product, spread_w, state, gate).astype(F32)
    normed = normalized(middle)
    return sent_operands(in_t, normed, deal), middle, gates(gate_w, normed)


def incoming_math(received, take, targets):
    blocks = [nn(take, received[128 * ka : 128 * ka + 128]) for ka in range(4)]
    swapped = [halves_swapped(blocks[0], blocks[1]), halves_swapped(blocks[2], blocks[3])]

    def side_of(place):
        rows = slice(32 * place, 32 * place + 32)
        return jnp.concatenate(
            [jnp.concatenate([half[rows] for half in pair], 0) for pair in swapped], 1
        ).astype(BF16)

    lefts = [nt(targets[channel], side_of(2 * channel)).astype(BF16) for channel in range(2)]
    right = jnp.concatenate([side_of(1), side_of(3)], 0)
    total = nn(jnp.concatenate(lefts, 1), right)
    blocks = []
    for k in (0, 128):
        blocks.extend(halves_swapped(total[0:256, k : k + 128], total[256:512, k : k + 128]))
    return jnp.concatenate(
        [b[64 * zh : 64 * zh + 64] for zh in range(4) for b in blocks], 0
    ).astype(BF16)


def last_math(gathered, state, gate, spread_w, eye):
    product = jnp.sum(gathered.astype(F32).reshape(4, 256, 128), axis=0)
    refined = residual(product, spread_w, state, gate)
    return jnp.concatenate([nt(eye, refined[0:128]), nt(eye, refined[128:256])], 0).astype(BF16)


def first_kernel(
    own_hbm, in_hbm, gate_hbm, out_hbm,
    sent, state, gate, next_in, gate_w, out_w, own, in_w, done,
):
    routes = (
        (own_hbm, own), (in_hbm.at[0], in_w),
        (gate_hbm, gate_w), (in_hbm.at[1], next_in), (out_hbm, out_w),
    )
    copies = [
        pltpu.make_async_copy(source, target, done.at[k])
        for k, (source, target) in enumerate(routes)
    ]
    for copy in copies:
        copy.start()
    row = lax.broadcasted_iota(jnp.int32, (256, 256), 0)
    col = lax.broadcasted_iota(jnp.int32, (256, 256), 1)
    deal = (col == row % 4 * 64 + row // 4).astype(F32).astype(BF16)
    for copy in copies[:3]:
        copy.wait()
    sent[...], state[...], gate[...] = first_math(
        own[...], in_w[...], gate_w[0], identity(), deal
    )
    for copy in copies[3:]:
        copy.wait()


def outgoing_kernel(received, out_w, moves, sent, spread_w):
    sent[...] = outgoing_math(received[...], moves[0:256], moves[256:512])
    spread_w[...] = spread_out(out_w[0], identity(), moves[512:768])


def middle_kernel(
    gathered, state, gate, spread_w, in_w, gate_w, deal, sent, middle, next_gate
):
    sent[...], middle[...], next_gate[...] = middle_math(
        gathered[...], state[...], gate[...], spread_w[...], in_w[...], gate_w[1], deal[...]
    )


def incoming_kernel(received, out_w, take, targets, moves, sent, spread_w):
    sent[...] = incoming_math(received[...], take[...], targets[...])
    spread_w[...] = spread_out(out_w[1], identity(), moves[512:768])


def last_kernel(gathered, state, gate, spread_w, refined):
    refined[...] = last_math(gathered[...], state[...], gate[...], spread_w[...], identity())


def call(kernel, outs, *arrays, space=pltpu.VMEM, scratch=()):
    vmem = pl.BlockSpec(memory_space=pltpu.VMEM)
    results = pl.pallas_call(
        kernel,
        out_shape=tuple(jax.ShapeDtypeStruct(shape, dtype) for shape, dtype in outs),
        in_specs=[pl.BlockSpec(memory_space=space)] * len(arrays),
        out_specs=tuple(vmem for _ in outs),
        scratch_shapes=scratch,
        compiler_params=pltpu.CompilerParams(
            vmem_limit_bytes=16 << 20
        ),
    )(*arrays)
    return results if len(results) > 1 else results[0]


def exchanged(rows, axes):
    blocks = rows.reshape(lax.axis_size(axes), -1, 128)
    return lax.all_to_all(blocks, axes, 0, 0, tiled=True).reshape(rows.shape)


def per_device(pair_rep, in_weights, gate_weights, out_weights):
    deal = jnp.asarray(DEAL)
    kept = ((256, 128), F32)
    wide = ((256, 256), BF16)
    moves = jnp.asarray(np.concatenate([SIDES, ROWS, *SPREAD], 0))
    inputs = [pair_rep.reshape(256, 128), in_weights, gate_weights, out_weights]
    squares = ((2, 128, 128), BF16)
    sent, state, gate, next_in, gate_w, out_w = call(
        first_kernel, [((512, 128), BF16), kept, kept, ((128, 512), BF16), squares, squares],
        *(pltpu.with_memory_space_constraint(v, pltpu.HBM) for v in inputs),
        space=pltpu.HBM,
        scratch=[
            pltpu.VMEM((256, 128), BF16), pltpu.VMEM((128, 512), BF16),
            pltpu.SemaphoreType.DMA((5,)),
        ],
    )
    sent, spread_w = call(
        outgoing_kernel, [((512, 128), BF16), wide], exchanged(sent, CHIPS), out_w, moves,
    )
    sent, state, gate = call(
        middle_kernel, [((512, 128), BF16), kept, kept],
        exchanged(sent, TO_OWNERS), state, gate, spread_w, next_in, gate_w, deal,
    )
    sent, spread_w = call(
        incoming_kernel, [((1024, 128), BF16), wide],
        exchanged(sent, LAYER), out_w,
        jnp.asarray(TAKE), jnp.asarray(TARGETS), moves,
    )
    refined = call(
        last_kernel, [((256, 128), BF16)],
        exchanged(sent, FROM_LAYER), state, gate, spread_w,
    )
    return refined.reshape(pair_rep.shape)


def solution(mesh):
    fine = Mesh(mesh.devices.reshape(4, 4, 4, 2, 2), ("y", "x", "zh", "zl", "c"))
    placed = P(("y", "x", "zh"), ("zl", "c"), None)
    return jax.shard_map(
        per_device, mesh=fine, in_specs=(placed, P(), P(), P()), out_specs=placed, check_vma=False
    )
```

```python
import jax
import jax.numpy as jnp
import numpy as np
from jax import lax
from jax.experimental import pallas as pl
from jax.experimental.pallas import tpu as pltpu
from jax.sharding import Mesh, PartitionSpec as P

EPSILON = 1e-05
BF16 = jnp.bfloat16
F32 = jnp.float32

CHIPS = ("zl", "y", "x", "zh")
TO_OWNERS = ("zl", "c", "y", "x", "zh")
LAYER = ("zl", "c", "y", "x")
FROM_LAYER = ("zh", "zl", "c", "y", "x")


def nn(a, b):
    return lax.dot_general(a, b, (((1,), (0,)), ((), ())), preferred_element_type=F32)


def nt(a, b):
    return lax.dot_general(a, b, (((1,), (1,)), ((), ())), preferred_element_type=F32)


def moved(one_hot, values):
    return nn(one_hot, values).astype(BF16)


def one_hot(rows, cols, source, valid=lambda i: i >= 0):
    index = np.arange(rows)
    hits = np.arange(cols)[None, :] == np.where(valid(index), source(index), -1)[:, None]
    return hits.astype(jnp.bfloat16)


DEAL = one_hot(256, 256, lambda i: i % 4 * 64 + i // 4)
SIDES = one_hot(256, 256, lambda i: i % 128 // 2 * 4 + i // 128 * 2 + i % 2)
ROWS = one_hot(256, 256, lambda i: i % 2 * 128 + i // 2)
TAKE = one_hot(128, 128, lambda i: i % 16 * 8 + i // 16)
TARGETS = np.stack(
    [
        one_hot(
            512, 256,
            lambda i: i % 64 // 4 * 16 + i % 256 // 64 * 4 + i % 2 * 2 + i // 256,
            lambda i: i // 2 % 2 == channel,
        )
        for channel in range(2)
    ]
)
SPREAD = np.stack(
    [one_hot(256, 128, lambda i: i // 2, lambda i: i % 2 == r).T for r in range(2)]
)


def identity():
    row = lax.broadcasted_iota(jnp.int32, (128, 128), 0)
    col = lax.broadcasted_iota(jnp.int32, (128, 128), 1)
    return (row == col).astype(F32).astype(BF16)


def normalized(values):
    tiles = values.reshape(-1, 128, 128)
    shifted = tiles - jnp.mean(tiles, axis=1, keepdims=True)
    spread = jnp.mean(shifted * shifted, axis=1, keepdims=True)
    return (shifted * lax.rsqrt(spread + EPSILON)).reshape(values.shape).astype(BF16)


def normalized_mixed(values):
    def mean(array):
        total = jnp.sum(array, axis=0)
        total = total + jnp.roll(total, 4, 0)
        return (total + jnp.roll(total, 2, 0)) / 128

    tiles = values.reshape(32, 8, 128)
    shifted = tiles - mean(tiles)
    scale = lax.rsqrt(mean(shifted * shifted) + EPSILON)
    return (shifted * scale).reshape(256, 128).astype(BF16)


def sigmoid(x):
    return 1.0 / (1.0 + jnp.exp(-x))


def halves_swapped(a, b):
    low = lax.broadcasted_iota(jnp.int32, a.shape, 1) < 64
    return jnp.where(low, a, jnp.roll(b, 64, 1)), jnp.where(low, jnp.roll(a, 64, 1), b)


def transposed(weights, eye):
    blocks = [nt(eye, weights[:, k : k + 128]) for k in range(0, weights.shape[1], 128)]
    return jnp.concatenate(blocks, 0).astype(BF16)


def sent_operands(weights, normed, deal):
    parts = []
    for r in range(2):
        projected = nn(weights, normed[128 * r : 128 * r + 128])
        for side in range(2):
            gate, value = (projected[k : k + 128] for k in (256 * side, 256 * side + 128))
            parts.append((sigmoid(gate) * value).astype(BF16))
    parts = [parts[k] for k in (0, 2, 1, 3)]
    return jnp.concatenate(
        [moved(deal, jnp.concatenate([p[k : k + 64] for p in parts], 0)) for k in (0, 64)], 0
    )


def gates(weights, state):
    normed = normalized(state)
    return jnp.concatenate([sigmoid(nn(weights, normed[k : k + 128])) for k in (0, 128)], 0)


def residual(product, spread_w, state, gate):
    update = nn(spread_w, normalized_mixed(product))
    return (state + gate * update).astype(BF16)


def first_math(own, in_w, eye, deal):
    state = jnp.concatenate([nt(eye, own[0:128]), nt(eye, own[128:256])], 0)
    return sent_operands(transposed(in_w, eye), normalized(state), deal), state


def spread_out(weights, eye, spread):
    weights = transposed(weights, eye)
    return jnp.concatenate([moved(weights, spread[0:128]), moved(weights, spread[128:256])], 0)


def outgoing_math(received, sides, rows):
    split = [nn(sides, received[256 * zl : 256 * zl + 256]) for zl in range(2)]
    left = [v.astype(BF16) for v in halves_swapped(split[0][0:128], split[1][0:128])]
    right = jnp.concatenate(halves_swapped(split[0][128:256], split[1][128:256]), 0)
    right = moved(rows, right.astype(BF16))
    even, odd = (nt(v, right) for v in left)
    blocks = []
    for k in (0, 128):
        blocks.extend(halves_swapped(even[:, k : k + 128], odd[:, k : k + 128]))
    return jnp.concatenate(blocks, 0).astype(BF16)


def middle_math(gathered, state, gate, spread_w, in_w, gate_w, deal):
    in_t = transposed(in_w, identity())
    parts = gathered.astype(F32).reshape(2, 2, 128, 128)
    product = (parts[:, 0] + parts[:, 1]).reshape(256, 128)
    middle = residual(product, spread_w, state, gate).astype(F32)
    normed = normalized(middle)
    gate_t = transposed(gate_w, identity())
    gate = [sigmoid(nn(gate_t, normed[k : k + 128])) for k in (0, 128)]
    return sent_operands(in_t, normed, deal), middle, jnp.concatenate(gate, 0)


def incoming_math(received, take, targets):
    blocks = [nn(take, received[128 * ka : 128 * ka + 128]) for ka in range(4)]
    swapped = [halves_swapped(blocks[0], blocks[1]), halves_swapped(blocks[2], blocks[3])]

    def side_of(place):
        rows = slice(32 * place, 32 * place + 32)
        return jnp.concatenate(
            [jnp.concatenate([half[rows] for half in pair], 0) for pair in swapped], 1
        ).astype(BF16)

    lefts = [nt(targets[channel], side_of(2 * channel)).astype(BF16) for channel in range(2)]
    right = jnp.concatenate([side_of(1), side_of(3)], 0)
    total = nn(jnp.concatenate(lefts, 1), right)
    blocks = []
    for k in (0, 128):
        blocks.extend(halves_swapped(total[0:256, k : k + 128], total[256:512, k : k + 128]))
    return jnp.concatenate(
        [b[64 * zh : 64 * zh + 64] for zh in range(4) for b in blocks], 0
    ).astype(BF16)


def last_math(gathered, state, gate, spread_w, eye):
    part = gathered.astype(F32).reshape(4, 256, 128)
    product = (part[0] + part[1]) + (part[2] + part[3])
    refined = residual(product, spread_w, state, gate)
    return jnp.concatenate([nt(eye, refined[0:128]), nt(eye, refined[128:256])], 0).astype(BF16)


def first_kernel(
    own_hbm, in_hbm, gate_hbm, out_hbm, sent, state, next_in, gate_w, out_w, own, in_w, done
):
    routes = (
        (own_hbm, own), (in_hbm.at[0], in_w),
        (in_hbm.at[1], next_in), (gate_hbm, gate_w), (out_hbm, out_w),
    )
    copies = [
        pltpu.make_async_copy(source, target, done.at[k])
        for k, (source, target) in enumerate(routes)
    ]
    for copy in copies:
        copy.start()
    row = lax.broadcasted_iota(jnp.int32, (256, 256), 0)
    col = lax.broadcasted_iota(jnp.int32, (256, 256), 1)
    deal = (col == row % 4 * 64 + row // 4).astype(F32).astype(BF16)
    for copy in copies[:2]:
        copy.wait()
    sent[...], state[...] = first_math(own[...], in_w[...], identity(), deal)
    for copy in copies[2:]:
        copy.wait()


def outgoing_kernel(received, state, gate_w, out_w, moves, sent, gate, spread_w):
    eye = identity()
    sent[...] = outgoing_math(received[...], moves[0:256], moves[256:512])
    gate[...] = gates(transposed(gate_w[0], eye), state[...])
    spread_w[...] = spread_out(out_w[0], eye, moves[512:768])


def middle_kernel(
    gathered, state, gate, spread_w, in_w, gate_w, deal, sent, middle, next_gate
):
    sent[...], middle[...], next_gate[...] = middle_math(
        gathered[...], state[...], gate[...], spread_w[...], in_w[...], gate_w[1], deal[...]
    )


def incoming_kernel(received, out_w, take, targets, moves, sent, spread_w):
    sent[...] = incoming_math(received[...], take[...], targets[...])
    spread_w[...] = spread_out(out_w[1], identity(), moves[512:768])


def last_kernel(gathered, state, gate, spread_w, refined):
    refined[...] = last_math(gathered[...], state[...], gate[...], spread_w[...], identity())


def call(kernel, outs, *arrays, space=pltpu.VMEM, scratch=()):
    vmem = pl.BlockSpec(memory_space=pltpu.VMEM)
    results = pl.pallas_call(
        kernel,
        out_shape=tuple(jax.ShapeDtypeStruct(shape, dtype) for shape, dtype in outs),
        in_specs=[pl.BlockSpec(memory_space=space)] * len(arrays),
        out_specs=tuple(vmem for _ in outs),
        scratch_shapes=scratch,
        compiler_params=pltpu.CompilerParams(
            vmem_limit_bytes=16 << 20
        ),
    )(*arrays)
    return results if len(results) > 1 else results[0]


def exchanged(rows, axes):
    blocks = rows.reshape(lax.axis_size(axes), -1, 128)
    return lax.all_to_all(blocks, axes, 0, 0, tiled=True).reshape(rows.shape)


def per_device(pair_rep, in_weights, gate_weights, out_weights):
    deal = jnp.asarray(DEAL)
    kept = ((256, 128), F32)
    wide = ((256, 256), BF16)
    moves = jnp.asarray(np.concatenate([SIDES, ROWS, *SPREAD], 0))
    inputs = [pair_rep.reshape(256, 128), in_weights, gate_weights, out_weights]
    squares = ((2, 128, 128), BF16)
    sent, state, next_in, gate_w, out_w = call(
        first_kernel, [((512, 128), BF16), kept, ((128, 512), BF16), squares, squares],
        *(pltpu.with_memory_space_constraint(v, pltpu.HBM) for v in inputs),
        space=pltpu.HBM,
        scratch=[
            pltpu.VMEM((256, 128), BF16), pltpu.VMEM((128, 512), BF16),
            pltpu.SemaphoreType.DMA((5,)),
        ],
    )
    sent, gate, spread_w = call(
        outgoing_kernel, [((512, 128), BF16), kept, wide],
        exchanged(sent, CHIPS), state, gate_w, out_w, moves,
    )
    sent, state, gate = call(
        middle_kernel, [((512, 128), BF16), kept, kept],
        exchanged(sent, TO_OWNERS), state, gate, spread_w, next_in, gate_w, deal,
    )
    sent, spread_w = call(
        incoming_kernel, [((1024, 128), BF16), wide],
        exchanged(sent, LAYER), out_w,
        jnp.asarray(TAKE), jnp.asarray(TARGETS), moves,
    )
    refined = call(
        last_kernel, [((256, 128), BF16)],
        exchanged(sent, FROM_LAYER), state, gate, spread_w,
    )
    return refined.reshape(pair_rep.shape)


def solution(mesh):
    fine = Mesh(mesh.devices.reshape(4, 4, 4, 2, 2), ("y", "x", "zh", "zl", "c"))
    placed = P(("y", "x", "zh"), ("zl", "c"), None)
    return jax.shard_map(
        per_device, mesh=fine, in_specs=(placed, P(), P(), P()), out_specs=placed, check_vma=False
    )
```
